256 devices in a mesh: tm: 16 (over x, z_lo, core), space: 16 (over z_hi, y).
Axes of the slice: x: 4, y: 4, z: 8 (z_hi: 4, z_lo: 2; z = z_hi * 2 + z_lo), core: 2. Of those that a mesh axis runs over, the one named last changes fastest.
Arguments:
- state_rhs: float32 [32, 32, 128, 128], P('tm', 'space'), may hold values from -5 to 9
- adjoint_rhs: float32 [32, 32, 128, 128], P('tm', 'space'), may hold values from -5 to 9
- reaction: float32 [32, 128, 128], P('space'), may hold values from 0.01 to 1
Outputs:
- state_out: float32 [32, 32, 128, 128], P('tm', 'space')
- adjoint_out: float32 [32, 32, 128, 128], P('tm', 'space')
The draws below stay inside these ranges and needn't reach their ends.
All inputs are finite; a program needn't handle non-finite values.
Results may differ from the reference program's by a relative error of at most 0.00021.
Values sent between devices are 32-bit elements; how exact they have to be, the bound alone decides.
A program may use at most 64 MiB of HBM per device.

```python
import math
import jax
import jax.numpy as jnp
from jax import lax

STEPS = 32
SWEEPS = 12
NX = 128
NY = 128
NZ = 32


def smooth_source(key, salt):
    folded = jax.random.fold_in(key, salt)
    phase_key, noise_key = jax.random.split(folded, 2)
    phases = jax.random.uniform(phase_key, (4,), jnp.float32, 0.0, 2.0 * math.pi)
    moments = jnp.arange(STEPS, dtype=jnp.float32)
    depths = jnp.arange(NZ, dtype=jnp.float32)
    across = jnp.arange(NX, dtype=jnp.float32)
    along = jnp.arange(NY, dtype=jnp.float32)
    amplitude = 1.5
    contrast = 0.4
    noise = jnp.clip(jax.random.normal(noise_key, (STEPS, NZ, NX, NY), jnp.float32), -5.0, 5.0)
    profile = 1.0 + 0.3 * jnp.cos(2.0 * math.pi * moments / STEPS + phases[0])
    strength = jnp.exp(contrast * jnp.cos(2.0 * math.pi * depths / 16.0 + phases[1]))
    lateral = 1.0 + 0.3 * jnp.cos(2.0 * math.pi * across / NX + phases[2])[:, None] * jnp.cos(2.0 * math.pi * along / NY + phases[3])[None, :]
    smooth = amplitude * profile[:, None, None, None] * strength[None, :, None, None] * lateral[None, None, :, :]
    return smooth + noise


def draw_state_rhs(key, part):
    return smooth_source(key, 11)


def draw_adjoint_rhs(key, part):
    return smooth_source(key, 23)


def draw_reaction(key, part):
    spread = jax.random.uniform(jax.random.fold_in(key, 37), (NZ, NX, NY), jnp.float32, 0.0, 1.0)
    return 0.01 * jnp.exp(math.log(100.0) * spread)


def setup_inputs(seed: int = 0) -> dict:
    arg_keys = jax.random.split(jax.random.key(seed), 4)
    return {
        "state_rhs": draw_state_rhs(jax.random.fold_in(arg_keys[3], 71), 0),
        "adjoint_rhs": draw_adjoint_rhs(jax.random.fold_in(arg_keys[3], 71), 0),
        "reaction": draw_reaction(jax.random.fold_in(arg_keys[3], 71), 0),
    }


ALPHA = 0.1
MU = 1.0
BETA = 1.0


def coefficients(reaction, freqs):
    turn = 2.0 * math.pi * freqs.astype(jnp.float32) / STEPS
    rate = math.exp(math.log(ALPHA) / STEPS)
    lam_re = 1.0 - rate * jnp.cos(turn)
    lam_im = rate * jnp.sin(turn)
    shaped = (-1,) + (1,) * reaction.ndim
    d_re = lam_re.reshape(shaped) + MU * (6.0 + reaction)
    d_im = jnp.broadcast_to(lam_im.reshape(shaped), d_re.shape)
    den_re = d_re * d_re - d_im * d_im + BETA * BETA
    den_im = 2.0 * d_re * d_im
    magnitude = den_re * den_re + den_im * den_im
    inv_re = den_re / magnitude
    inv_im = -den_im / magnitude
    return (d_re * inv_re - d_im * inv_im, d_re * inv_im + d_im * inv_re, BETA * inv_re, BETA * inv_im)


def block_solve(coefficient, source):
    q_re, q_im, r_re, r_im = coefficient
    y_real = source[..., 0, :, :, :]
    y_imag = source[..., 1, :, :, :]
    p_real = source[..., 2, :, :, :]
    p_imag = source[..., 3, :, :, :]
    new_yre = q_re * y_real - q_im * y_imag + (r_re * p_real - r_im * p_imag)
    new_yim = q_re * y_imag + q_im * y_real + (r_re * p_imag + r_im * p_real)
    new_pre = q_re * p_real - q_im * p_imag - (r_re * y_real - r_im * y_imag)
    new_pim = q_re * p_imag + q_im * p_real - (r_re * y_imag + r_im * y_real)
    return jnp.stack((new_yre, new_yim, new_pre, new_pim), axis=-4)


def neighbour_sum(field):
    padded = jnp.pad(field, ((0, 0), (1, 1), (1, 1), (1, 1)))
    total = padded[:, 2:, 1:-1, 1:-1] + padded[:, :-2, 1:-1, 1:-1]
    total = total + padded[:, 1:-1, 2:, 1:-1] + padded[:, 1:-1, :-2, 1:-1]
    return total + padded[:, 1:-1, 1:-1, 2:] + padded[:, 1:-1, 1:-1, :-2]


def reference(state_rhs, adjoint_rhs, reaction):
    times = jnp.arange(STEPS, dtype=jnp.float32)
    growth = jnp.exp(math.log(ALPHA) * times / STEPS)[:, None, None, None]
    shrink = jnp.exp(-math.log(ALPHA) * times / STEPS)[:, None, None, None]
    state_hat = jnp.fft.fft(state_rhs * growth, axis=0)
    adjoint_hat = jnp.fft.fft(adjoint_rhs[::-1] * growth, axis=0)
    sources = jnp.stack((state_hat.real, state_hat.imag, adjoint_hat.real, adjoint_hat.imag), axis=1)

    def solve_one(inputs):
        freq_rhs, freq_index = inputs
        coefficient = tuple(member[0] for member in coefficients(reaction, freq_index[None]))
        field = block_solve(coefficient, freq_rhs)

        def sweep(sweep_index, current):
            return block_solve(coefficient, freq_rhs + MU * neighbour_sum(current))

        return lax.fori_loop(0, SWEEPS - 1, sweep, field)

    solved = lax.map(solve_one, (sources, jnp.arange(STEPS, dtype=jnp.int32)))
    state_back = jnp.fft.ifft(solved[:, 0] + 1j * solved[:, 1], axis=0).real * shrink
    adjoint_back = (jnp.fft.ifft(solved[:, 2] + 1j * solved[:, 3], axis=0).real * shrink)[::-1]
    return state_back, adjoint_back
```

```python
import math

import jax
import jax.numpy as jnp
from jax import lax
from jax.experimental import pallas as pl
from jax.experimental.pallas import tpu as pltpu
from jax.sharding import PartitionSpec as P

STEPS = 32
SWEEPS = 12
ALPHA = 0.1
MESH = pl.DeviceIdType.MESH
HALO = 8
TAIL = 3
ROWS = 16 + 2 * HALO
F32 = jnp.float32


def device(x, z, core, y):
    return (x * 4 + (z % 2) * 2 + core, (z // 2) * 4 + y)


def mul_const(v, c):
    re, im = v
    cr, ci = c.real, c.imag
    if abs(ci) < 1e-12:
        if abs(cr - 1.0) < 1e-12:
            return v
        return (re * cr, im * cr)
    if abs(cr) < 1e-12:
        if abs(ci - 1.0) < 1e-12:
            return (-im, re)
        if abs(ci + 1.0) < 1e-12:
            return (im, -re)
        return (im * (-ci), re * ci)
    return (re * cr - im * ci, re * ci + im * cr)


def add(a, b):
    return (a[0] + b[0], a[1] + b[1])


def sub(a, b):
    return (a[0] - b[0], a[1] - b[1])


def small_dft(values, sign):
    n = len(values)
    if n == 1:
        return values
    even = small_dft(values[0::2], sign)
    odd = small_dft(values[1::2], sign)
    out = [None] * n
    for k in range(n // 2):
        angle = sign * 2.0 * math.pi * k / n
        t = mul_const(odd[k], complex(math.cos(angle), math.sin(angle)))
        out[k] = add(even[k], t)
        out[k + n // 2] = sub(even[k], t)
    return out


def long_dft(load, store, tmp, sign):
    for b in range(8):
        group = small_dft([load(8 * a + b) for a in range(4)], sign)
        for k1 in range(4):
            angle = sign * 2.0 * math.pi * b * k1 / 32
            re, im = mul_const(group[k1], complex(math.cos(angle), math.sin(angle)))
            tmp[8 * k1 + b, 0] = re
            tmp[8 * k1 + b, 1] = im
    for k1 in range(4):
        group = small_dft([(tmp[8 * k1 + b, 0], tmp[8 * k1 + b, 1]) for b in range(8)], sign)
        for k2 in range(8):
            store(k1 + 4 * k2, group[k2])


def kernel(
    state, adjoint, reaction, out,
    src, rsrc, r1, rf, rh, b1, tmp, f1, fld, fh, s, w, u0, u1, hal, g, f2, b2,
    load_sem, send_sem, recv_sem,
):
    tm = lax.axis_index("tm")
    sp = lax.axis_index("space")
    x, zlo, core = tm // 4, (tm // 2) % 2, tm % 2
    zhi, y = sp // 4, sp % 4
    z = zhi * 2 + zlo
    zhh, par = zhi // 2, zhi % 2
    zp, rtl = x // 2, x % 2
    freq = x * 8 + y * 2 + core
    zlow = core * 8 + y * 2 + zp
    up, down = (z + 1) % 8, (z + 7) % 8
    home = core == par

    loads = [
        pltpu.make_async_copy(reaction, rsrc, load_sem.at[2]),
        pltpu.make_async_copy(state, src.at[0], load_sem.at[0]),
        pltpu.make_async_copy(adjoint, src.at[1], load_sem.at[1]),
    ]
    for c in loads:
        c.start()

    barrier = pltpu.get_barrier_semaphore()

    def greet(dev):
        pl.semaphore_signal(barrier, inc=1, device_id=dev, device_id_type=MESH)

    def greet_plane(i, _):
        xx, zz = (x + i // 8) % 4, (z + i) % 8
        here = jnp.logical_and(home, i == 0)

        @pl.when(jnp.logical_not(here))
        def _():
            greet(device(xx, zz, par, y))

        return 0

    lax.fori_loop(0, 32, greet_plane, 0)

    def source_of(i):
        xx, cc, ll = (x + i // 8) % 4, (core + (i // 4) % 2) % 2, (zlo + (i // 2) % 2) % 2
        hh = (zhh + i % 2) % 2
        return xx, (core + 2 * hh) * 2 + ll, cc, hh

    def greet_source(i, _):
        xx, zz, cc, hh = source_of(i)
        here = jnp.logical_and(home, i == 0)

        @pl.when(jnp.logical_not(here))
        def _():
            greet(device(xx, zz, cc, y))

        return 0

    lax.fori_loop(0, 32, greet_source, 0)

    def mate(i):
        return (x + i // 8) % 4, (y + (i // 2) % 4) % 4, (core + i % 2) % 2

    def greet_mate(i, _):
        xx, yy, cc = mate(i)
        greet(device(xx, z, cc, yy))
        return 0

    lax.fori_loop(1, 32, greet_mate, 0)
    greet(device(x, up, core, y))
    greet(device(x, down, core, y))
    pl.semaphore_wait(barrier, 97 - 2 * home.astype(jnp.int32))

    def copy_to(src_ref, dst_ref, phase, dev):
        return pltpu.make_async_remote_copy(
            src_ref=src_ref, dst_ref=dst_ref, send_sem=send_sem.at[phase],
            recv_sem=recv_sem.at[phase], device_id=dev, device_id_type=MESH,
        )

    def copy_here(src_ref, dst_ref, phase):
        return pltpu.make_async_copy(src_ref, dst_ref, recv_sem.at[phase])

    def arrived(ref, phase):
        pltpu.make_async_copy(ref, ref, recv_sem.at[phase]).wait()

    def sent(ref, phase):
        pltpu.make_async_copy(ref, ref, send_sem.at[phase]).wait()

    loads[0].wait()
    for i in range(2):
        zz = zlo * 4 + core * 2 + i
        tile = rsrc.at[zp, 2 * zz + rtl]
        here = jnp.logical_and(home, zz == z)

        @pl.when(here)
        def _():
            copy_here(tile, r1.at[zhh], 0).start()

        @pl.when(jnp.logical_not(here))
        def _():
            copy_to(tile, r1.at[zhh], 0, device(x, zz, par, y)).start()

    loads[1].wait()
    loads[2].wait()

    def first(i, _):
        xx, zz = (x + i // 8) % 4, (z + i) % 8
        piece = src.at[:, :, xx // 2, 2 * zz + xx % 2]
        place = b1.at[zhh, :, pl.ds(2 * tm, 2)]
        here = jnp.logical_and(home, i == 0)

        @pl.when(here)
        def _():
            copy_here(piece, place, 1).start()

        @pl.when(jnp.logical_not(here))
        def _():
            copy_to(piece, place, 1, device(xx, zz, par, y)).start()

        return 0

    lax.fori_loop(0, 32, first, 0)

    arrived(r1, 0)
    copy_here(r1, rf.at[:, zlow, rtl], 2).start()

    def spread_reaction(i, _):
        xx, yy, cc = mate(i)
        copy_to(r1, rf.at[:, zlow, rtl], 2, device(xx, z, cc, yy)).start()
        return 0

    lax.fori_loop(1, 32, spread_reaction, 0)
    arrived(rf, 2)
    copy_to(rf.at[:, :, 0], rh.at[1], 3, device(x, down, core, y)).start()
    copy_to(rf.at[:, :, 1], rh.at[0], 4, device(x, up, core, y)).start()

    cos_k, sin_k = jnp.float32(0.0), jnp.float32(0.0)
    for k in range(STEPS):
        angle = 2.0 * math.pi * k / STEPS
        cos_k = jnp.where(freq == k, jnp.float32(math.cos(angle)), cos_k)
        sin_k = jnp.where(freq == k, jnp.float32(math.sin(angle)), sin_k)
    rate = math.exp(math.log(ALPHA) / STEPS)
    base_re = 1.0 - rate * cos_k + 6.0
    d_im = rate * sin_k + 1.0

    def coefficient(row, j, value, keep):
        d_re = base_re + value
        inv = 1.0 / (d_re * d_re + d_im * d_im)
        w_re = d_re * inv
        w_im = -d_im * inv
        if keep is not None:
            w_re = jnp.where(keep, w_re, 0.0)
            w_im = jnp.where(keep, w_im, 0.0)
        w[row, 0, j] = w_re
        w[row, 1, j] = w_im

    rfl = rf.reshape(512, 128)
    rhl = rh.reshape(512, 128)

    def inner_rows(r, _):
        for t in range(2):
            for j in range(4):
                value = rfl[pl.ds(j * 16 + t * 8 + r, 8, stride=64), :]
                coefficient(HALO + t * 8 + r, j, value, None)
        return 0

    lax.fori_loop(0, 8, inner_rows, 0)

    arrived(b1, 1)
    for tile in range(2):

        def load(n):
            growth = math.exp(math.log(ALPHA) * n / STEPS)
            return (b1[tile, 0, n] * growth, b1[tile, 1, STEPS - 1 - n] * growth)

        def store(k, v):
            f1[k, tile, 0] = v[0]
            f1[k, tile, 1] = v[1]

        long_dft(load, store, tmp, -1)

    def second(i, _):
        xx, yy, cc = mate(i)
        copy_to(f1.at[xx * 8 + yy * 2 + cc], fld.at[:, zlow, rtl], 5, device(xx, z, cc, yy)).start()
        return 0

    copy_here(f1.at[freq], fld.at[:, zlow, rtl], 5).start()
    lax.fori_loop(1, 32, second, 0)

    arrived(rh.at[1], 3)
    arrived(rh.at[0], 4)

    def outer_rows(r, _):
        for side in range(2):
            keep = (z > 0) if side == 0 else (z < 7)
            for j in range(4):
                value = rhl[pl.ds(side * 256 + j * 8 + r, 8, stride=32), :]
                coefficient(side * (HALO + 16) + r, j, value, keep)
        return 0

    lax.fori_loop(0, 8, outer_rows, 0)

    arrived(fld, 5)
    copy_to(fld.at[:, :, 0], fh.at[1], 6, device(x, down, core, y)).start()
    copy_to(fld.at[:, :, 1], fh.at[0], 7, device(x, up, core, y)).start()

    fll = fld.reshape(1024, 128)
    fhl = fh.reshape(1024, 128)

    def start_row(row, j, v):
        s[row, 0, j] = v[0]
        s[row, 1, j] = v[1]
        w_re, w_im = w[row, 0, j], w[row, 1, j]
        u0[row, 0, j] = w_re * v[0] - w_im * v[1]
        u0[row, 1, j] = w_re * v[1] + w_im * v[0]

    def inner_start(r, _):
        for t in range(2):
            for j in range(4):
                v = [fll[pl.ds(j * 32 + t * 16 + c * 8 + r, 8, stride=128), :] for c in range(2)]
                start_row(HALO + t * 8 + r, j, v)
        return 0

    lax.fori_loop(0, 8, inner_start, 0)
    arrived(fh.at[1], 6)
    arrived(fh.at[0], 7)

    def outer_start(r, _):
        for side in range(2):
            for j in range(4):
                v = [fhl[pl.ds(side * 512 + j * 16 + c * 8 + r, 8, stride=64), :] for c in range(2)]
                start_row(side * (HALO + 16) + r, j, v)
        return 0

    lax.fori_loop(0, 8, outer_start, 0)

    lanes = lax.broadcasted_iota(jnp.int32, (8, 128), 1)
    subs = lax.broadcasted_iota(jnp.int32, (8, 128), 0)
    first_lane, last_lane = lanes == 0, lanes == 127
    first_sub, last_sub = subs == 0, subs == 7

    def sweep_row(old, new, row):
        total = [[None] * 4, [None] * 4]
        for c in range(2):
            mid = [old[row, c, j] for j in range(4)]
            before = jnp.where(first_sub, 0.0, pltpu.roll(mid[3], 1, 0))
            after = jnp.where(last_sub, 0.0, pltpu.roll(mid[0], 7, 0))
            line = [before] + mid + [after]
            for j in range(4):
                t = s[row, c, j] + (line[j] + line[j + 2])
                t = t + (old[row - 1, c, j] + old[row + 1, c, j])
                left = jnp.where(first_lane, 0.0, pltpu.roll(mid[j], 1, 1))
                right = jnp.where(last_lane, 0.0, pltpu.roll(mid[j], 127, 1))
                total[c][j] = t + (left + right)
        for j in range(4):
            w_re, w_im = w[row, 0, j], w[row, 1, j]
            t_re, t_im = total[0][j], total[1][j]
            new[row, 0, j] = w_re * t_re - w_im * t_im
            new[row, 1, j] = w_re * t_im + w_im * t_re

    def sweep(old, new, low, high):
        count = high - low

        def four(i, _):
            for k in range(4):
                sweep_row(old, new, low + 4 * i + k)
            return 0

        lax.fori_loop(0, count // 4, four, 0)
        for row in range(low + count // 4 * 4, high):
            sweep_row(old, new, row)

    pair = [u0, u1]
    for m in range(1, HALO + 1):
        sweep(pair[(m + 1) % 2], pair[m % 2], m, ROWS - m)
    last = pair[HALO % 2]
    copy_to(last.at[pl.ds(HALO, TAIL)], hal.at[1], 8, device(x, down, core, y)).start()
    copy_to(last.at[pl.ds(HALO + 16 - TAIL, TAIL)], hal.at[0], 9, device(x, up, core, y)).start()
    arrived(hal.at[1], 8)
    arrived(hal.at[0], 9)
    for k in range(TAIL):
        for c in range(2):
            for j in range(4):
                last[HALO - TAIL + k, c, j] = jnp.where(z > 0, hal[0, k, c, j], 0.0)
                last[HALO + 16 + k, c, j] = jnp.where(z < 7, hal[1, k, c, j], 0.0)
    for m in range(HALO + 1, SWEEPS):
        margin = SWEEPS - 1 - m
        if m == HALO + 2:
            sent(hal.at[1], 8)
            sent(hal.at[0], 9)
        sweep(pair[(m + 1) % 2], pair[m % 2], HALO - margin, HALO + 16 + margin)
    result = pair[(SWEEPS - 1) % 2]

    gl = g.reshape(1024, 128)

    def turn_back(r, _):
        for t in range(2):
            for j in range(4):
                for c in range(2):
                    gl[pl.ds(j * 32 + t * 16 + c * 8 + r, 8, stride=128), :] = result[HALO + t * 8 + r, c, j]
        return 0

    lax.fori_loop(0, 8, turn_back, 0)

    def third(i, _):
        xx, yy, cc = mate(i)
        piece = g.at[:, cc * 8 + yy * 2 + xx // 2, xx % 2]
        copy_to(piece, f2.at[freq], 10, device(xx, z, cc, yy)).start()
        return 0

    copy_here(g.at[:, zlow, rtl], f2.at[freq], 10).start()
    lax.fori_loop(1, 32, third, 0)
    arrived(f2, 10)

    for tile in range(2):

        def load(k):
            return (f2[k, tile, 0], f2[k, tile, 1])

        def store(n, v):
            shrink = math.exp(-math.log(ALPHA) * n / STEPS) / STEPS
            b2[tile, 0, n] = v[0] * shrink
            b2[tile, 1, STEPS - 1 - n] = v[1] * shrink

        long_dft(load, store, tmp, 1)

    def fourth(i, _):
        xx, zz, cc, hh = source_of(i)
        times = pl.ds(2 * (xx * 4 + (zz % 2) * 2 + cc), 2)
        piece = b2.at[hh, :, times]
        place = out.at[:, :, zp, 2 * z + rtl]
        here = jnp.logical_and(home, i == 0)

        @pl.when(here)
        def _():
            copy_here(piece, place, 11).start()

        @pl.when(jnp.logical_not(here))
        def _():
            copy_to(piece, place, 11, device(xx, zz, cc, y)).start()

        return 0

    lax.fori_loop(0, 32, fourth, 0)

    for i in range(2):
        zz = zlo * 4 + core * 2 + i

        @pl.when(jnp.logical_not(jnp.logical_and(home, zz == z)))
        def _():
            sent(r1.at[0], 0)

    sent(rh.at[1], 3)
    sent(rh.at[0], 4)
    sent(fh.at[1], 6)
    sent(fh.at[0], 7)

    def drain(i, _):
        sent(r1, 2)
        sent(f1.at[0], 5)
        sent(f2.at[0], 10)
        sent(f1.at[0], 1)
        sent(f1.at[0], 11)
        return 0

    lax.fori_loop(1, 32, drain, 0)

    @pl.when(jnp.logical_not(home))
    def _():
        sent(f1.at[0], 1)
        sent(f1.at[0], 11)

    arrived(out, 11)


def body(state_rhs, adjoint_rhs, reaction):
    tile = (8, 128)
    field = pltpu.VMEM((ROWS, 2, 4) + tile, F32)
    result = pl.pallas_call(
        kernel,
        out_shape=jax.ShapeDtypeStruct((2, 2, 2, 16) + tile, F32),
        in_specs=[pl.BlockSpec(memory_space=pl.ANY)] * 3,
        out_specs=pl.BlockSpec(memory_space=pl.ANY),
        scratch_shapes=[
            pltpu.VMEM((2, 2, 2, 16) + tile, F32),
            pltpu.VMEM((2, 16) + tile, F32),
            pltpu.VMEM((2,) + tile, F32),
            pltpu.VMEM((2, 16, 2) + tile, F32),
            pltpu.VMEM((2, 2, 16) + tile, F32),
            pltpu.VMEM((2, 2, 32) + tile, F32),
            pltpu.VMEM((32, 2) + tile, F32),
            pltpu.VMEM((32, 2, 2) + tile, F32),
            pltpu.VMEM((2, 16, 2, 2) + tile, F32),
            pltpu.VMEM((2, 2, 16, 2) + tile, F32),
            field,
            field,
            field,
            field,
            pltpu.VMEM((2, TAIL, 2, 4) + tile, F32),
            pltpu.VMEM((2, 16, 2, 2) + tile, F32),
            pltpu.VMEM((32, 2, 2) + tile, F32),
            pltpu.VMEM((2, 2, 32) + tile, F32),
            pltpu.SemaphoreType.DMA((3,)),
            pltpu.SemaphoreType.DMA((12,)),
            pltpu.SemaphoreType.DMA((12,)),
        ],
        compiler_params=pltpu.CompilerParams(collective_id=0, has_side_effects=True),
        name="precondition",
    )(
        state_rhs.reshape((2, 2, 16) + tile),
        adjoint_rhs.reshape((2, 2, 16) + tile),
        reaction.reshape((2, 16) + tile),
    )
    return (result[0].reshape(state_rhs.shape), result[1].reshape(state_rhs.shape))


def solution(mesh):
    placed = P("tm", "space", None, None)
    return jax.shard_map(
        body,
        mesh=mesh,
        in_specs=(placed, placed, P("space", None, None)),
        out_specs=(placed, placed),
        check_vma=False,
    )
```

```python
import math

import jax
import jax.numpy as jnp
from jax import lax
from jax.experimental import pallas as pl
from jax.experimental.pallas import tpu as pltpu
from jax.sharding import PartitionSpec as P

STEPS = 32
SWEEPS = 12
ALPHA = 0.1
MESH = pl.DeviceIdType.MESH
TAIL = 3
HALO = 8 + TAIL
ROWS = 16 + 2 * HALO
BLOCK = 8
F32 = jnp.float32


def rem(a, n):
    return lax.rem(a, jnp.int32(n))


def div(a, n):
    return lax.div(a, jnp.int32(n))


def mul_const(v, c):
    re, im = v
    cr, ci = c.real, c.imag
    if abs(ci) < 1e-12:
        if abs(cr - 1.0) < 1e-12:
            return v
        return (re * cr, im * cr)
    if abs(cr) < 1e-12:
        if abs(ci - 1.0) < 1e-12:
            return (-im, re)
        if abs(ci + 1.0) < 1e-12:
            return (im, -re)
        return (im * (-ci), re * ci)
    return (re * cr - im * ci, re * ci + im * cr)


def add(a, b):
    return (a[0] + b[0], a[1] + b[1])


def sub(a, b):
    return (a[0] - b[0], a[1] - b[1])


def small_dft(values, sign):
    n = len(values)
    if n == 1:
        return values
    even = small_dft(values[0::2], sign)
    odd = small_dft(values[1::2], sign)
    out = [None] * n
    for k in range(n // 2):
        angle = sign * 2.0 * math.pi * k / n
        t = mul_const(odd[k], complex(math.cos(angle), math.sin(angle)))
        out[k] = add(even[k], t)
        out[k + n // 2] = sub(even[k], t)
    return out


def long_dft(load, store, tmp, sign):
    for b in range(8):
        group = small_dft([load(8 * a + b) for a in range(4)], sign)
        for k1 in range(4):
            angle = sign * 2.0 * math.pi * b * k1 / 32
            re, im = mul_const(group[k1], complex(math.cos(angle), math.sin(angle)))
            tmp[8 * k1 + b, 0] = re
            tmp[8 * k1 + b, 1] = im
    for k1 in range(4):
        group = small_dft([(tmp[8 * k1 + b, 0], tmp[8 * k1 + b, 1]) for b in range(8)], sign)
        for k2 in range(8):
            store(k1 + 4 * k2, group[k2])


def kernel(
    state, adjoint, reaction, out,
    src, rsrc, r1, rf, rha, rhb, b1, tmp, f1, fld, fha, fhb, s, w, u0, u1, g, f2, b2,
    load_sem, send_sem, recv_sem, group_sem,
):
    tm = lax.axis_index("tm")
    sp = lax.axis_index("space")
    x, zlo, core = div(tm, 4), rem(div(tm, 2), 2), rem(tm, 2)
    zhi, y = div(sp, 4), rem(sp, 4)
    z = zhi * 2 + zlo
    zhh, par = div(zhi, 2), rem(zhi, 2)
    zp, rtl = div(x, 2), rem(x, 2)
    freq = x * 8 + y * 2 + core
    home = core == par
    away = jnp.logical_not(home)

    loads = [
        pltpu.make_async_copy(reaction, rsrc, load_sem.at[2]),
        pltpu.make_async_copy(state, src.at[0], load_sem.at[0]),
        pltpu.make_async_copy(adjoint, src.at[1], load_sem.at[1]),
    ]
    for c in loads:
        c.start()

    xs = [rem(x + i, 4) for i in range(4)]
    ys = [rem(y + i, 4) for i in range(4)]
    cs = [core, 1 - core]
    zs = [rem(z + i, 8) for i in range(8)]
    hs = [zhh, 1 - zhh]
    ls = [zlo, 1 - zlo]
    z_tm = [rem(v, 2) * 2 for v in zs]
    z_sp = [div(v, 2) * 4 for v in zs]

    def plane(ix, iz):
        return (xs[ix] * 4 + z_tm[iz] + par, z_sp[iz] + y)

    def mate(ix, iy, ic):
        return (xs[ix] * 4 + zlo * 2 + cs[ic], zhi * 4 + ys[iy])

    def origin(ix, il, ic, h):
        return (xs[ix] * 4 + ls[il] * 2 + cs[ic], (core + 2 * h) * 4 + y)

    above = (x * 4 + z_tm[1] + core, z_sp[1] + y)
    below = (x * 4 + z_tm[7] + core, z_sp[7] + y)
    far_first = (4, 3, 5, 2, 6, 1, 7, 0)
    near_first = (0, 1, 7, 2, 6, 3, 5, 4)
    across = (2, 1, 3, 0)

    def near(cc):
        return div(rem(z - 2 * cc + 9, 8), 4)

    barrier = pltpu.get_barrier_semaphore()

    def greet(dev):
        pl.semaphore_signal(barrier, inc=1, device_id=dev, device_id_type=MESH)

    for iz in far_first:
        for ix in across:
            if ix or iz:
                greet(plane(ix, iz))
    for ih in (1, 0):
        for ix in across:
            for il in (1, 0):
                for ic in (1, 0):
                    if ix or il or ic or ih:
                        greet(origin(ix, il, ic, hs[ih]))
    for iy in across:
        for ix in across:
            for ic in (1, 0):
                if ix or iy or ic:
                    greet(mate(ix, iy, ic))
    greet(above)
    greet(below)

    @pl.when(away)
    def _():
        greet(plane(0, 0))
        greet(origin(0, 0, 0, zhh))

    pl.semaphore_wait(barrier, 97 - 2 * home.astype(jnp.int32))

    def copy_to(src_ref, dst_ref, phase, dev, sem=None):
        return pltpu.make_async_remote_copy(
            src_ref=src_ref, dst_ref=dst_ref, send_sem=send_sem.at[phase],
            recv_sem=recv_sem.at[phase] if sem is None else sem,
            device_id=dev, device_id_type=MESH,
        )

    def wait_on(ref, sem):
        pltpu.make_async_copy(ref, ref, sem).wait()

    def arrived(ref, phase):
        wait_on(ref, recv_sem.at[phase])

    def sent(ref, phase):
        wait_on(ref, send_sem.at[phase])

    loads[0].wait()
    for i in range(2):
        zz = zlo * 4 + core * 2 + i
        tile = rsrc.at[zp, 2 * zz + rtl]
        here = jnp.logical_and(home, zz == z)

        @pl.when(here)
        def _():
            pltpu.make_async_copy(tile, r1.at[zhh], recv_sem.at[0]).start()

        @pl.when(jnp.logical_not(here))
        def _():
            dev = (x * 4 + rem(zz, 2) * 2 + par, div(zz, 2) * 4 + y)
            copy_to(tile, r1.at[zhh], 0, dev).start()

    loads[1].wait()
    loads[2].wait()

    place = b1.at[zhh, :, pl.ds(2 * tm, 2)]
    b1_sem = recv_sem.at[1 + zhh]

    def piece(ix, iz):
        return src.at[:, :, div(xs[ix], 2), 2 * zs[iz] + rem(xs[ix], 2)]

    @pl.when(home)
    def _():
        pltpu.make_async_copy(piece(0, 0), place, b1_sem).start()

    @pl.when(away)
    def _():
        copy_to(piece(0, 0), place, 1, plane(0, 0), b1_sem).start()

    for iz in near_first:
        for ix in across:
            if ix or iz:
                copy_to(piece(ix, iz), place, 1, plane(ix, iz), b1_sem).start()

    arrived(r1, 0)
    pltpu.make_async_copy(r1, rf.at[:, core, y, zp, rtl], recv_sem.at[3]).start()
    for iy in across:
        for ix in across:
            for ic in (1, 0):
                if ix or iy or ic:
                    copy_to(r1, rf.at[:, core, y, zp, rtl], 3, mate(ix, iy, ic)).start()

    def transform(tile):
        def load(n):
            growth = math.exp(math.log(ALPHA) * n / STEPS)
            return (b1[tile, 0, n] * growth, b1[tile, 1, STEPS - 1 - n] * growth)

        def store(k, v):
            f1[k, tile, 0] = v[0]
            f1[k, tile, 1] = v[1]

        long_dft(load, store, tmp, -1)

    def second(tile, half):
        goal = fld.at[tile, core, y, zp, rtl]
        for iy in across:
            for ix in across:
                for ic in (1, 0):
                    if ix or iy or ic:
                        k = xs[ix] * 8 + ys[iy] * 2 + cs[ic]
                        copy_to(f1.at[k, tile], goal, 4, mate(ix, iy, ic), group_sem.at[half, iy]).start()
        pltpu.make_async_copy(f1.at[freq, tile], goal, group_sem.at[half, 0]).start()

    def pass_on(half):
        for iy in across:
            yy = ys[(4 - iy) % 4]
            wait_on(fld.at[0, :, yy], group_sem.at[half, iy])
            for cc in range(2):
                tile = near(cc) if half == 0 else 1 - near(cc)
                at = (tile, cc, yy)
                got = fld.at[at]
                copy_to(got.at[:, 0], fha.at[(1,) + at], 5, below).start()
                copy_to(got.at[:, 1], fha.at[(0,) + at], 6, above).start()
                copy_to(got.at[:, 1, :, pl.ds(0, TAIL)], fhb.at[(1,) + at].at[:, :, :TAIL], 7, below).start()
                copy_to(got.at[:, 0, :, pl.ds(8 - TAIL, TAIL)], fhb.at[(0,) + at].at[:, :, :TAIL], 8, above).start()

    close = near(core)
    arrived(b1.at[0], 1 + close)
    transform(close)
    second(close, 0)

    arrived(rf, 3)
    cos_k, sin_k = jnp.float32(0.0), jnp.float32(0.0)
    for k in range(STEPS):
        angle = 2.0 * math.pi * k / STEPS
        cos_k = jnp.where(freq == k, jnp.float32(math.cos(angle)), cos_k)
        sin_k = jnp.where(freq == k, jnp.float32(math.sin(angle)), sin_k)
    rate = math.exp(math.log(ALPHA) / STEPS)
    base_re = 1.0 - rate * cos_k + 6.0
    d_im = rate * sin_k + 1.0

    def coefficient(row, j, value, keep):
        d_re = base_re + value
        inv = 1.0 / (d_re * d_re + d_im * d_im)
        w_re = d_re * inv
        w_im = -d_im * inv
        if keep is not None:
            w_re = jnp.where(keep, w_re, 0.0)
            w_im = jnp.where(keep, w_im, 0.0)
        w[row, 0, j] = w_re
        w[row, 1, j] = w_im

    rfl = rf.reshape(512, 128)
    ral = rha.reshape(512, 128)
    rbl = rhb.reshape(512, 128)

    def inner_rows(r, _):
        for t in range(2):
            for j in range(4):
                value = rfl[pl.ds(j * 16 + t * 8 + r, 8, stride=64), :]
                coefficient(HALO + t * 8 + r, j, value, None)
        return 0

    lax.fori_loop(0, 8, inner_rows, 0)

    arrived(b1.at[0], 2 - close)
    transform(1 - close)
    second(1 - close, 1)
    copy_to(rf.at[:, :, :, :, 0], rha.at[1], 9, below).start()
    copy_to(rf.at[:, :, :, :, 1], rha.at[0], 10, above).start()
    copy_to(rf.at[:, :, :, :, 1, pl.ds(0, TAIL)], rhb.at[1, :, :, :, :, :TAIL], 11, below).start()
    copy_to(rf.at[:, :, :, :, 0, pl.ds(8 - TAIL, TAIL)], rhb.at[0, :, :, :, :, :TAIL], 12, above).start()
    pass_on(0)
    for side in range(2):
        arrived(rha.at[side], 10 - side)
        arrived(rhb.at[side, :, :, :, :, :TAIL], 12 - side)

    def outer_rows(side, r, at, flat):
        keep = (z > 0) if side == 0 else (z < 7)
        for j in range(4):
            value = flat[pl.ds(side * 256 + j * 8 + at, 8, stride=32), :]
            coefficient(r, j, value, keep)

    def wide_rows(r, _):
        outer_rows(0, TAIL + r, r, ral)
        outer_rows(1, HALO + 16 + r, r, ral)
        return 0

    lax.fori_loop(0, 8, wide_rows, 0)
    for r in range(TAIL):
        outer_rows(0, r, r, rbl)
        outer_rows(1, HALO + 24 + r, r, rbl)

    pass_on(1)

    fll = fld.reshape(1024, 128)
    fal = fha.reshape(1024, 128)
    fbl = fhb.reshape(1024, 128)

    def start_row(row, j, v):
        s[row, 0, j] = v[0]
        s[row, 1, j] = v[1]
        w_re, w_im = w[row, 0, j], w[row, 1, j]
        u0[row, 0, j] = w_re * v[0] - w_im * v[1]
        u0[row, 1, j] = w_re * v[1] + w_im * v[0]

    def inner_start(r, _):
        for t in range(2):
            for j in range(4):
                v = [fll[pl.ds(j * 32 + t * 16 + c * 8 + r, 8, stride=128), :] for c in range(2)]
                start_row(HALO + t * 8 + r, j, v)
        return 0

    lax.fori_loop(0, 8, inner_start, 0)
    for side in range(2):
        arrived(fha.at[side], 6 - side)
        arrived(fhb.at[side, :, :, :, :, :, :TAIL], 8 - side)

    def outer_start(side, row, at, flat):
        for j in range(4):
            first = side * 512 + j * 16 + at
            v = [flat[pl.ds(first + c * 8, 8, stride=64), :] for c in range(2)]
            start_row(row, j, v)

    def wide_start(r, _):
        outer_start(0, TAIL + r, r, fal)
        outer_start(1, HALO + 16 + r, r, fal)
        return 0

    lax.fori_loop(0, 8, wide_start, 0)
    for r in range(TAIL):
        outer_start(0, r, r, fbl)
        outer_start(1, HALO + 24 + r, r, fbl)

    lanes = lax.broadcasted_iota(jnp.int32, (8, 128), 1)
    subs = lax.broadcasted_iota(jnp.int32, (8, 128), 0)
    first_lane, last_lane = lanes == 0, lanes == 127
    first_sub, last_sub = subs == 0, subs == 7

    def sweep_row(old, new, row):
        total = [[None] * 4, [None] * 4]
        for c in range(2):
            mid = [old[row, c, j] for j in range(4)]
            before = jnp.where(first_sub, 0.0, pltpu.roll(mid[3], 1, 0))
            after = jnp.where(last_sub, 0.0, pltpu.roll(mid[0], 7, 0))
            line = [before] + mid + [after]
            for j in range(4):
                t = s[row, c, j] + (line[j] + line[j + 2])
                t = t + (old[row - 1, c, j] + old[row + 1, c, j])
                left = jnp.where(first_lane, 0.0, pltpu.roll(mid[j], 1, 1))
                right = jnp.where(last_lane, 0.0, pltpu.roll(mid[j], 127, 1))
                total[c][j] = t + (left + right)
        for j in range(4):
            w_re, w_im = w[row, 0, j], w[row, 1, j]
            t_re, t_im = total[0][j], total[1][j]
            new[row, 0, j] = w_re * t_re - w_im * t_im
            new[row, 1, j] = w_re * t_im + w_im * t_re

    def sweep(old, new, low, high):
        count = high - low

        def block(i, _):
            start = jnp.minimum(low + BLOCK * i, high - BLOCK)
            for k in range(BLOCK):
                sweep_row(old, new, start + k)
            return 0

        lax.fori_loop(0, (count + BLOCK - 1) // BLOCK, block, 0)

    pair = [u0, u1]
    for m in range(1, SWEEPS):
        sweep(pair[(m + 1) % 2], pair[m % 2], m, ROWS - m)
    result = pair[(SWEEPS - 1) % 2]

    gl = g.reshape(1024, 128)

    def turn_back(r, _):
        for t in range(2):
            for j in range(4):
                for c in range(2):
                    gl[pl.ds(j * 32 + t * 16 + c * 8 + r, 8, stride=128), :] = result[HALO + t * 8 + r, c, j]
        return 0

    lax.fori_loop(0, 8, turn_back, 0)

    for half in range(2):
        tiles = [1 - near(cc) if half == 0 else near(cc) for cc in cs]
        for iy in across:
            for ix in across:
                for ic in (1, 0):
                    if ix or iy or ic:
                        part = g.at[tiles[ic], cs[ic], ys[iy], div(xs[ix], 2), rem(xs[ix], 2)]
                        copy_to(part, f2.at[tiles[ic], freq], 13, mate(ix, iy, ic), recv_sem.at[14 + half]).start()
        own = g.at[tiles[0], core, y, zp, rtl]
        pltpu.make_async_copy(own, f2.at[tiles[0], freq], recv_sem.at[14 + half]).start()

    def transform_back(tile):
        def load(k):
            return (f2[tile, k, 0], f2[tile, k, 1])

        def store(n, v):
            shrink = math.exp(-math.log(ALPHA) * n / STEPS) / STEPS
            b2[tile, 0, n] = v[0] * shrink
            b2[tile, 1, STEPS - 1 - n] = v[1] * shrink

        long_dft(load, store, tmp, 1)

    goal = out.at[:, :, zp, 2 * z + rtl]

    def fourth(tile):
        for ix in across:
            for il in (1, 0):
                for ic in (1, 0):
                    times = pl.ds(2 * (xs[ix] * 4 + ls[il] * 2 + cs[ic]), 2)
                    part = b2.at[tile, :, times]
                    dev = origin(ix, il, ic, tile)
                    if ix or il or ic:
                        copy_to(part, goal, 16, dev).start()
                    else:
                        here = jnp.logical_and(home, tile == zhh)

                        @pl.when(here)
                        def _():
                            pltpu.make_async_copy(part, goal, recv_sem.at[16]).start()

                        @pl.when(jnp.logical_not(here))
                        def _():
                            copy_to(part, goal, 16, dev).start()

    arrived(f2.at[0], 14)
    transform_back(1 - close)
    fourth(1 - close)
    arrived(f2.at[0], 15)
    transform_back(close)
    fourth(close)

    for i in range(2):
        zz = zlo * 4 + core * 2 + i

        @pl.when(jnp.logical_not(jnp.logical_and(home, zz == z)))
        def _():
            sent(r1.at[0], 0)

    for side in range(2):
        sent(fha.at[side], 6 - side)
        sent(fhb.at[side, :, :, :, :, :, :TAIL], 8 - side)
        sent(rha.at[side], 10 - side)
        sent(rhb.at[side, :, :, :, :, :TAIL], 12 - side)

    def drain(i, _):
        sent(b1.at[0, :, pl.ds(0, 2)], 1)
        sent(r1, 3)
        sent(f1.at[0], 4)
        sent(f1.at[0], 13)
        sent(b1.at[0, :, pl.ds(0, 2)], 16)
        return 0

    lax.fori_loop(1, 32, drain, 0)

    @pl.when(away)
    def _():
        sent(b1.at[0, :, pl.ds(0, 2)], 1)
        sent(b1.at[0, :, pl.ds(0, 2)], 16)

    arrived(out, 16)


def body(state_rhs, adjoint_rhs, reaction):
    tile = (8, 128)
    planes = (2, 2, 4, 2)
    field = pltpu.VMEM((ROWS, 2, 4) + tile, F32)
    result = pl.pallas_call(
        kernel,
        out_shape=jax.ShapeDtypeStruct((2, 2, 2, 16) + tile, F32),
        in_specs=[pl.BlockSpec(memory_space=pl.ANY)] * 3,
        out_specs=pl.BlockSpec(memory_space=pl.ANY),
        scratch_shapes=[
            pltpu.VMEM((2, 2, 2, 16) + tile, F32),
            pltpu.VMEM((2, 16) + tile, F32),
            pltpu.VMEM((2,) + tile, F32),
            pltpu.VMEM(planes + (2,) + tile, F32),
            pltpu.VMEM((2,) + planes + tile, F32),
            pltpu.VMEM((2,) + planes + tile, F32),
            pltpu.VMEM((2, 2, 32) + tile, F32),
            pltpu.VMEM((32, 2) + tile, F32),
            pltpu.VMEM((32, 2, 2) + tile, F32),
            pltpu.VMEM(planes + (2, 2) + tile, F32),
            pltpu.VMEM((2,) + planes + (2,) + tile, F32),
            pltpu.VMEM((2,) + planes + (2,) + tile, F32),
            field,
            field,
            field,
            field,
            pltpu.VMEM(planes + (2, 2) + tile, F32),
            pltpu.VMEM((2, 32, 2) + tile, F32),
            pltpu.VMEM((2, 2, 32) + tile, F32),
            pltpu.SemaphoreType.DMA((3,)),
            pltpu.SemaphoreType.DMA((17,)),
            pltpu.SemaphoreType.DMA((17,)),
            pltpu.SemaphoreType.DMA((2, 4)),
        ],
        compiler_params=pltpu.CompilerParams(collective_id=0, has_side_effects=True),
        name="precondition",
    )(
        state_rhs.reshape((2, 2, 16) + tile),
        adjoint_rhs.reshape((2, 2, 16) + tile),
        reaction.reshape((2, 16) + tile),
    )
    return (result[0].reshape(state_rhs.shape), result[1].reshape(state_rhs.shape))


def solution(mesh):
    placed = P("tm", "space", None, None)
    return jax.shard_map(
        body,
        mesh=mesh,
        in_specs=(placed, placed, P("space", None, None)),
        out_specs=(placed, placed),
        check_vma=False,
    )
```

```python
import math

import jax
import jax.numpy as jnp
from jax import lax
from jax.experimental import pallas as pl
from jax.experimental.pallas import tpu as pltpu
from jax.sharding import PartitionSpec as P

STEPS = 32
SWEEPS = 12
ALPHA = 0.1
MESH = pl.DeviceIdType.MESH
TAIL = 3
HALO = 8 + TAIL
ROWS = 16 + 2 * HALO
F32 = jnp.float32


def rem(a, n):
    return lax.rem(a, jnp.int32(n))


def div(a, n):
    return lax.div(a, jnp.int32(n))


def mul_const(v, c):
    re, im = v
    cr, ci = c.real, c.imag
    if abs(ci) < 1e-12:
        if abs(cr - 1.0) < 1e-12:
            return v
        return (re * cr, im * cr)
    if abs(cr) < 1e-12:
        if abs(ci - 1.0) < 1e-12:
            return (-im, re)
        if abs(ci + 1.0) < 1e-12:
            return (im, -re)
        return (im * (-ci), re * ci)
    return (re * cr - im * ci, re * ci + im * cr)


def add(a, b):
    return (a[0] + b[0], a[1] + b[1])


def sub(a, b):
    return (a[0] - b[0], a[1] - b[1])


def small_dft(values, sign):
    n = len(values)
    if n == 1:
        return values
    even = small_dft(values[0::2], sign)
    odd = small_dft(values[1::2], sign)
    out = [None] * n
    for k in range(n // 2):
        angle = sign * 2.0 * math.pi * k / n
        t = mul_const(odd[k], complex(math.cos(angle), math.sin(angle)))
        out[k] = add(even[k], t)
        out[k + n // 2] = sub(even[k], t)
    return out


def long_dft(load, store, tmp, sign):
    for b in range(8):
        group = small_dft([load(8 * a + b) for a in range(4)], sign)
        for k1 in range(4):
            angle = sign * 2.0 * math.pi * b * k1 / 32
            re, im = mul_const(group[k1], complex(math.cos(angle), math.sin(angle)))
            tmp[8 * k1 + b, 0] = re
            tmp[8 * k1 + b, 1] = im
    for k1 in range(4):
        group = small_dft([(tmp[8 * k1 + b, 0], tmp[8 * k1 + b, 1]) for b in range(8)], sign)
        for k2 in range(8):
            store(k1 + 4 * k2, group[k2])


def kernel(
    state, adjoint, reaction, out,
    src, rsrc, r1, rf, b1, tmp, f1, fld, fha, fhb, s, w, u, g, f2, b2,
    load_sem, send_sem, recv_sem, group_sem,
):
    tm = lax.axis_index("tm")
    sp = lax.axis_index("space")
    x, zlo, core = div(tm, 4), rem(div(tm, 2), 2), rem(tm, 2)
    zhi, y = div(sp, 4), rem(sp, 4)
    z = zhi * 2 + zlo
    zhh, par = div(zhi, 2), rem(zhi, 2)
    zp, rtl = rem(x, 2), div(x, 2)
    freq = x * 8 + y * 2 + core
    home = core == par
    away = jnp.logical_not(home)

    loads = [
        pltpu.make_async_copy(reaction, rsrc.at[:, 2:18], load_sem.at[2]),
        pltpu.make_async_copy(reaction.at[:, 14:16], rsrc.at[:, 0:2], load_sem.at[3]),
        pltpu.make_async_copy(reaction.at[:, 0:2], rsrc.at[:, 18:20], load_sem.at[4]),
        pltpu.make_async_copy(state, src.at[0], load_sem.at[0]),
        pltpu.make_async_copy(adjoint, src.at[1], load_sem.at[1]),
    ]
    for c in loads:
        c.start()

    xs = [rem(x + i, 4) for i in range(4)]
    ys = [rem(y + i, 4) for i in range(4)]
    cs = [core, 1 - core]
    zs = [rem(z + i, 8) for i in range(8)]
    hs = [zhh, 1 - zhh]
    ls = [zlo, 1 - zlo]
    z_tm = [rem(v, 2) * 2 for v in zs]
    z_sp = [div(v, 2) * 4 for v in zs]

    def plane(ix, iz):
        return (xs[ix] * 4 + z_tm[iz] + par, z_sp[iz] + y)

    def mate(ix, iy, ic):
        return (xs[ix] * 4 + zlo * 2 + cs[ic], zhi * 4 + ys[iy])

    def origin(ix, il, ic, h):
        return (xs[ix] * 4 + ls[il] * 2 + cs[ic], (core + 2 * h) * 4 + y)

    above = (x * 4 + z_tm[1] + core, z_sp[1] + y)
    below = (x * 4 + z_tm[7] + core, z_sp[7] + y)
    far_first = (4, 3, 5, 2, 6, 1, 7, 0)
    near_first = (0, 1, 7, 2, 6, 3, 5, 4)
    across = (2, 1, 3, 0)

    def near(cc):
        return div(rem(z - 2 * cc + 9, 8), 4)

    barrier = pltpu.get_barrier_semaphore()

    def greet(dev):
        pl.semaphore_signal(barrier, inc=1, device_id=dev, device_id_type=MESH)

    for iz in far_first:
        for ix in across:
            if ix or iz:
                greet(plane(ix, iz))
    for ih in (1, 0):
        for ix in across:
            for il in (1, 0):
                for ic in (1, 0):
                    if ix or il or ic or ih:
                        greet(origin(ix, il, ic, hs[ih]))
    for iy in across:
        for ix in across:
            for ic in (1, 0):
                if ix or iy or ic:
                    greet(mate(ix, iy, ic))
    greet(above)
    greet(below)

    @pl.when(away)
    def _():
        greet(plane(0, 0))
        greet(origin(0, 0, 0, zhh))

    pl.semaphore_wait(barrier, 97 - 2 * home.astype(jnp.int32))

    def copy_to(src_ref, dst_ref, phase, dev, sem=None):
        return pltpu.make_async_remote_copy(
            src_ref=src_ref, dst_ref=dst_ref, send_sem=send_sem.at[phase],
            recv_sem=recv_sem.at[phase] if sem is None else sem,
            device_id=dev, device_id_type=MESH,
        )

    def wait_on(ref, sem):
        pltpu.make_async_copy(ref, ref, sem).wait()

    def arrived(ref, phase):
        wait_on(ref, recv_sem.at[phase])

    def sent(ref, phase):
        wait_on(ref, send_sem.at[phase])

    for c in loads[:3]:
        c.wait()
    for i in range(2):
        zz = zlo * 4 + core * 2 + i
        here = jnp.logical_and(home, zz == z)
        rows = rsrc.at[zp, pl.ds(2 * zz, 6)]

        @pl.when(here)
        def _():
            pltpu.make_async_copy(rows, r1.at[zhh], recv_sem.at[0]).start()

        @pl.when(jnp.logical_not(here))
        def _():
            dev = (x * 4 + rem(zz, 2) * 2 + par, div(zz, 2) * 4 + y)
            copy_to(rows, r1.at[zhh], 0, dev).start()

    for c in loads[3:]:
        c.wait()

    place = b1.at[zhh, :, pl.ds(2 * tm, 2)]
    b1_sem = recv_sem.at[1 + zhh]

    def piece(ix, iz):
        return src.at[:, :, rem(xs[ix], 2), 2 * zs[iz] + div(xs[ix], 2)]

    @pl.when(home)
    def _():
        pltpu.make_async_copy(piece(0, 0), place, b1_sem).start()

    @pl.when(away)
    def _():
        copy_to(piece(0, 0), place, 1, plane(0, 0), b1_sem).start()

    for iz in near_first:
        for ix in across:
            if ix or iz:
                copy_to(piece(ix, iz), place, 1, plane(ix, iz), b1_sem).start()

    def transform(tile):
        def load(n):
            growth = math.exp(math.log(ALPHA) * n / STEPS)
            return (b1[tile, 0, n] * growth, b1[tile, 1, STEPS - 1 - n] * growth)

        def store(k, v):
            f1[k, tile, 0] = v[0]
            f1[k, tile, 1] = v[1]

        long_dft(load, store, tmp, -1)

    def second(tile, half):
        goal = fld.at[tile, core, y, zp, rtl]
        for iy in across:
            for ix in across:
                for ic in (1, 0):
                    if ix or iy or ic:
                        k = xs[ix] * 8 + ys[iy] * 2 + cs[ic]
                        copy_to(f1.at[k, tile], goal, 4, mate(ix, iy, ic), group_sem.at[half, iy]).start()
        pltpu.make_async_copy(f1.at[freq, tile], goal, group_sem.at[half, 0]).start()

    def shared(half, iy):
        yy = ys[(4 - iy) % 4]
        for cc in range(2):
            tile = near(cc) if half == 0 else 1 - near(cc)
            yield (tile, cc, yy)

    def pass_on(half):
        for iy in across:
            wait_on(fld.at[0, :, ys[(4 - iy) % 4]], group_sem.at[half, iy])
            for at in shared(half, iy):
                got = fld.at[at]
                copy_to(got.at[:, 0], fha.at[(1,) + at], 5, below).start()
                copy_to(got.at[:, 1], fha.at[(0,) + at], 6, above).start()

    def pass_rest():
        for half in range(2):
            for iy in across:
                for at in shared(half, iy):
                    got = fld.at[at]
                    copy_to(got.at[:, 1, :, pl.ds(0, TAIL)], fhb.at[(1,) + at].at[:, :, :TAIL], 7, below).start()
                    copy_to(got.at[:, 0, :, pl.ds(8 - TAIL, TAIL)], fhb.at[(0,) + at].at[:, :, :TAIL], 8, above).start()

    arrived(r1, 0)
    half_rf = rf.at[:, core]
    beside = rem(x + 1 + 2 * rem(y, 2), 4)
    for iy in across:
        copy_to(r1, half_rf.at[:, y, zp], 3, (beside * 4 + zlo * 2 + core, zhi * 4 + ys[iy])).start()
    for iy in across[:3]:
        copy_to(r1, half_rf.at[:, y, zp], 3, mate(0, iy, 0)).start()
    pltpu.make_async_copy(r1, half_rf.at[:, y, zp], recv_sem.at[3]).start()

    close = near(core)
    arrived(b1.at[0], 1 + close)
    transform(close)
    second(close, 0)

    arrived(rf.at[:, 0], 3)
    copy_to(half_rf, half_rf, 9, mate(0, 0, 1)).start()
    arrived(b1.at[0], 2 - close)
    transform(1 - close)
    second(1 - close, 1)
    pass_on(0)
    arrived(rf.at[:, 0], 9)
    cos_k, sin_k = jnp.float32(0.0), jnp.float32(0.0)
    for k in range(STEPS):
        angle = 2.0 * math.pi * k / STEPS
        cos_k = jnp.where(freq == k, jnp.float32(math.cos(angle)), cos_k)
        sin_k = jnp.where(freq == k, jnp.float32(math.sin(angle)), sin_k)
    rate = math.exp(math.log(ALPHA) / STEPS)
    base_re = 1.0 - rate * cos_k + 6.0
    d_im = rate * sin_k + 1.0

    def coefficient(row, j, value, keep):
        d_re = base_re + value
        inv = 1.0 / (d_re * d_re + d_im * d_im)
        w_re = d_re * inv
        w_im = -d_im * inv
        if keep is not None:
            w_re = jnp.where(keep, w_re, 0.0)
            w_im = jnp.where(keep, w_im, 0.0)
        w[row, 0, j] = w_re
        w[row, 1, j] = w_im

    rfl = rf.reshape(1536, 128)

    def coefficient_row(row, keep):
        for j in range(4):
            value = rfl[pl.ds(j * 48 + row + 16 - HALO, 8, stride=192), :]
            coefficient(row, j, value, keep)

    def coefficient_rows(r, _):
        coefficient_row(HALO + r, None)
        coefficient_row(HALO + 8 + r, None)
        coefficient_row(TAIL + r, z > 0)
        coefficient_row(HALO + 16 + r, z < 7)
        return 0

    lax.fori_loop(0, 8, coefficient_rows, 0)
    for r in range(TAIL):
        coefficient_row(r, z > 0)
        coefficient_row(HALO + 24 + r, z < 7)

    pass_on(1)
    pass_rest()

    fll = fld.reshape(1024, 128)
    fal = fha.reshape(1024, 128)
    fbl = fhb.reshape(1024, 128)

    def start_row(row, j, v):
        s[row, 0, j] = v[0]
        s[row, 1, j] = v[1]
        w_re, w_im = w[row, 0, j], w[row, 1, j]
        u[0, row, 0, j] = w_re * v[0] - w_im * v[1]
        u[0, row, 1, j] = w_re * v[1] + w_im * v[0]

    def inner_start(r, _):
        for t in range(2):
            for j in range(4):
                v = [fll[pl.ds(j * 32 + t * 16 + c * 8 + r, 8, stride=128), :] for c in range(2)]
                start_row(HALO + t * 8 + r, j, v)
        return 0

    lax.fori_loop(0, 8, inner_start, 0)
    lanes = lax.broadcasted_iota(jnp.int32, (8, 128), 1)
    subs = lax.broadcasted_iota(jnp.int32, (8, 128), 0)
    first_lane, last_lane = lanes == 0, lanes == 127
    first_sub, last_sub = subs == 0, subs == 7

    def sweep_row(m, row):
        total = [[None] * 4, [None] * 4]
        for c in range(2):
            mid = [u[m - 1, row, c, j] for j in range(4)]
            before = jnp.where(first_sub, 0.0, pltpu.roll(mid[3], 1, 0))
            after = jnp.where(last_sub, 0.0, pltpu.roll(mid[0], 7, 0))
            line = [before] + mid + [after]
            for j in range(4):
                t = s[row, c, j] + (line[j] + line[j + 2])
                t = t + (u[m - 1, row - 1, c, j] + u[m - 1, row + 1, c, j])
                left = jnp.where(first_lane, 0.0, pltpu.roll(mid[j], 1, 1))
                right = jnp.where(last_lane, 0.0, pltpu.roll(mid[j], 127, 1))
                total[c][j] = t + (left + right)
        for j in range(4):
            w_re, w_im = w[row, 0, j], w[row, 1, j]
            t_re, t_im = total[0][j], total[1][j]
            u[m, row, 0, j] = w_re * t_re - w_im * t_im
            u[m, row, 1, j] = w_re * t_im + w_im * t_re

    done = [set() for _ in range(SWEEPS)]

    def sweeps(edge):
        for m in range(1, SWEEPS):
            rows = set(range(edge + m, ROWS - edge - m)) - done[m]
            done[m] |= rows
            for row in sorted(rows):
                sweep_row(m, row)

    sweeps(HALO)
    for side in range(2):
        arrived(fha.at[side], 6 - side)

    def outer_start(side, row, at, flat):
        for j in range(4):
            first = side * 512 + j * 16 + at
            v = [flat[pl.ds(first + c * 8, 8, stride=64), :] for c in range(2)]
            start_row(row, j, v)

    def wide_start(r, _):
        outer_start(0, TAIL + r, r, fal)
        outer_start(1, HALO + 16 + r, r, fal)
        return 0

    lax.fori_loop(0, 8, wide_start, 0)
    sweeps(TAIL)
    for side in range(2):
        arrived(fhb.at[side, :, :, :, :, :, :TAIL], 8 - side)
    for r in range(TAIL):
        outer_start(0, r, r, fbl)
        outer_start(1, HALO + 24 + r, r, fbl)
    sweeps(0)

    gl = g.reshape(1024, 128)

    def turn_back(r, _):
        for t in range(2):
            for j in range(4):
                for c in range(2):
                    gl[pl.ds(j * 32 + t * 16 + c * 8 + r, 8, stride=128), :] = u[SWEEPS - 1, HALO + t * 8 + r, c, j]
        return 0

    lax.fori_loop(0, 8, turn_back, 0)

    for half in range(2):
        tiles = [1 - near(cc) if half == 0 else near(cc) for cc in cs]
        for iy in across:
            for ix in across:
                for ic in (1, 0):
                    if ix or iy or ic:
                        part = g.at[tiles[ic], cs[ic], ys[iy], rem(xs[ix], 2), div(xs[ix], 2)]
                        copy_to(part, f2.at[tiles[ic], freq], 13, mate(ix, iy, ic), recv_sem.at[14 + half]).start()
        own = g.at[tiles[0], core, y, zp, rtl]
        pltpu.make_async_copy(own, f2.at[tiles[0], freq], recv_sem.at[14 + half]).start()

    def transform_back(tile):
        def load(k):
            return (f2[tile, k, 0], f2[tile, k, 1])

        def store(n, v):
            shrink = math.exp(-math.log(ALPHA) * n / STEPS) / STEPS
            b2[tile, 0, n] = v[0] * shrink
            b2[tile, 1, STEPS - 1 - n] = v[1] * shrink

        long_dft(load, store, tmp, 1)

    goal = out.at[:, :, zp, 2 * z + rtl]

    def fourth(tile):
        for ix in across:
            for il in (1, 0):
                for ic in (1, 0):
                    times = pl.ds(2 * (xs[ix] * 4 + ls[il] * 2 + cs[ic]), 2)
                    part = b2.at[tile, :, times]
                    dev = origin(ix, il, ic, tile)
                    if ix or il or ic:
                        copy_to(part, goal, 16, dev).start()
                    else:
                        here = jnp.logical_and(home, tile == zhh)

                        @pl.when(here)
                        def _():
                            pltpu.make_async_copy(part, goal, recv_sem.at[16]).start()

                        @pl.when(jnp.logical_not(here))
                        def _():
                            copy_to(part, goal, 16, dev).start()

    arrived(f2.at[0], 14)
    transform_back(1 - close)
    fourth(1 - close)
    arrived(f2.at[0], 15)
    transform_back(close)
    fourth(close)

    for i in range(2):
        zz = zlo * 4 + core * 2 + i

        @pl.when(jnp.logical_not(jnp.logical_and(home, zz == z)))
        def _():
            sent(r1.at[0], 0)

    for side in range(2):
        sent(fha.at[side], 6 - side)
        sent(fhb.at[side, :, :, :, :, :, :TAIL], 8 - side)

    sent(rf.at[:, 0], 9)

    def drain_reaction(i, _):
        sent(r1, 3)
        return 0

    lax.fori_loop(1, 8, drain_reaction, 0)

    def drain(i, _):
        sent(b1.at[0, :, pl.ds(0, 2)], 1)
        sent(f1.at[0], 4)
        sent(f1.at[0], 13)
        sent(b1.at[0, :, pl.ds(0, 2)], 16)
        return 0

    lax.fori_loop(1, 32, drain, 0)

    @pl.when(away)
    def _():
        sent(b1.at[0, :, pl.ds(0, 2)], 1)
        sent(b1.at[0, :, pl.ds(0, 2)], 16)

    arrived(out, 16)


def body(state_rhs, adjoint_rhs, reaction):
    tile = (8, 128)
    planes = (2, 2, 4, 2)
    field = pltpu.VMEM((ROWS, 2, 4) + tile, F32)
    result = pl.pallas_call(
        kernel,
        out_shape=jax.ShapeDtypeStruct((2, 2, 2, 16) + tile, F32),
        in_specs=[pl.BlockSpec(memory_space=pl.ANY)] * 3,
        out_specs=pl.BlockSpec(memory_space=pl.ANY),
        scratch_shapes=[
            pltpu.VMEM((2, 2, 2, 16) + tile, F32),
            pltpu.VMEM((2, 20) + tile, F32),
            pltpu.VMEM((2, 6) + tile, F32),
            pltpu.VMEM(planes + (6,) + tile, F32),
            pltpu.VMEM((2, 2, 32) + tile, F32),
            pltpu.VMEM((32, 2) + tile, F32),
            pltpu.VMEM((32, 2, 2) + tile, F32),
            pltpu.VMEM(planes + (2, 2) + tile, F32),
            pltpu.VMEM((2,) + planes + (2,) + tile, F32),
            pltpu.VMEM((2,) + planes + (2,) + tile, F32),
            field,
            field,
            pltpu.VMEM((SWEEPS, ROWS, 2, 4) + tile, F32),
            pltpu.VMEM(planes + (2, 2) + tile, F32),
            pltpu.VMEM((2, 32, 2) + tile, F32),
            pltpu.VMEM((2, 2, 32) + tile, F32),
            pltpu.SemaphoreType.DMA((5,)),
            pltpu.SemaphoreType.DMA((17,)),
            pltpu.SemaphoreType.DMA((17,)),
            pltpu.SemaphoreType.DMA((2, 4)),
        ],
        compiler_params=pltpu.CompilerParams(collective_id=0, has_side_effects=True),
        name="precondition",
    )(
        state_rhs.reshape((2, 2, 16) + tile),
        adjoint_rhs.reshape((2, 2, 16) + tile),
        reaction.reshape((2, 16) + tile),
    )
    return (result[0].reshape(state_rhs.shape), result[1].reshape(state_rhs.shape))


def solution(mesh):
    placed = P("tm", "space", None, None)
    return jax.shard_map(
        body,
        mesh=mesh,
        in_specs=(placed, placed, P("space", None, None)),
        out_specs=(placed, placed),
        check_vma=False,
    )
```

```python
import math

import jax
import jax.numpy as jnp
from jax import lax
from jax.experimental import pallas as pl
from jax.experimental.pallas import tpu as pltpu
from jax.sharding import PartitionSpec as P

STEPS = 32
SWEEPS = 12
ALPHA = 0.1
MESH = pl.DeviceIdType.MESH
TAIL = 3
HALO = 8 + TAIL
ROWS = 16 + 2 * HALO
F32 = jnp.float32


def rem(a, n):
    return lax.rem(a, jnp.int32(n))


def div(a, n):
    return lax.div(a, jnp.int32(n))


def mul_const(v, c):
    re, im = v
    cr, ci = c.real, c.imag
    if abs(ci) < 1e-12:
        if abs(cr - 1.0) < 1e-12:
            return v
        return (re * cr, im * cr)
    if abs(cr) < 1e-12:
        if abs(ci - 1.0) < 1e-12:
            return (-im, re)
        if abs(ci + 1.0) < 1e-12:
            return (im, -re)
        return (im * (-ci), re * ci)
    return (re * cr - im * ci, re * ci + im * cr)


def add(a, b):
    return (a[0] + b[0], a[1] + b[1])


def sub(a, b):
    return (a[0] - b[0], a[1] - b[1])


def small_dft(values, sign):
    n = len(values)
    if n == 1:
        return values
    even = small_dft(values[0::2], sign)
    odd = small_dft(values[1::2], sign)
    out = [None] * n
    for k in range(n // 2):
        angle = sign * 2.0 * math.pi * k / n
        t = mul_const(odd[k], complex(math.cos(angle), math.sin(angle)))
        out[k] = add(even[k], t)
        out[k + n // 2] = sub(even[k], t)
    return out


def long_dft(load, store, tmp, sign):
    for b in range(8):
        group = small_dft([load(8 * a + b) for a in range(4)], sign)
        for k1 in range(4):
            angle = sign * 2.0 * math.pi * b * k1 / 32
            re, im = mul_const(group[k1], complex(math.cos(angle), math.sin(angle)))
            tmp[8 * k1 + b, 0] = re
            tmp[8 * k1 + b, 1] = im
    for k1 in range(4):
        group = small_dft([(tmp[8 * k1 + b, 0], tmp[8 * k1 + b, 1]) for b in range(8)], sign)
        for k2 in range(8):
            store(k1 + 4 * k2, group[k2])


def kernel(
    state, adjoint, reaction, out,
    src, rsrc, r1, rf, b1, tmp, f1, fld, fha, fhb, s, w, u, g, f2, b2,
    load_sem, send_sem, recv_sem, group_sem,
):
    tm = lax.axis_index("tm")
    sp = lax.axis_index("space")
    x, zlo, core = div(tm, 4), rem(div(tm, 2), 2), rem(tm, 2)
    zhi, y = div(sp, 4), rem(sp, 4)
    z = zhi * 2 + zlo
    zhh, par = div(zhi, 2), rem(zhi, 2)
    zp, rtl = rem(x, 2), div(x, 2)
    freq = x * 8 + y * 2 + core
    home = core == par
    away = jnp.logical_not(home)

    loads = [
        pltpu.make_async_copy(reaction, rsrc.at[:, 2:18], load_sem.at[2]),
        pltpu.make_async_copy(reaction.at[:, 14:16], rsrc.at[:, 0:2], load_sem.at[3]),
        pltpu.make_async_copy(reaction.at[:, 0:2], rsrc.at[:, 18:20], load_sem.at[4]),
        pltpu.make_async_copy(state, src.at[0], load_sem.at[0]),
        pltpu.make_async_copy(adjoint, src.at[1], load_sem.at[1]),
    ]
    for c in loads:
        c.start()

    xs = [rem(x + i, 4) for i in range(4)]
    ys = [rem(y + i, 4) for i in range(4)]
    cs = [core, 1 - core]
    zs = [rem(z + i, 8) for i in range(8)]
    hs = [zhh, 1 - zhh]
    ls = [zlo, 1 - zlo]
    z_tm = [rem(v, 2) * 2 for v in zs]
    z_sp = [div(v, 2) * 4 for v in zs]

    def plane(ix, iz):
        return (xs[ix] * 4 + z_tm[iz] + par, z_sp[iz] + y)

    def mate(ix, iy, ic):
        return (xs[ix] * 4 + zlo * 2 + cs[ic], zhi * 4 + ys[iy])

    def origin(ix, il, ic, h):
        return (xs[ix] * 4 + ls[il] * 2 + cs[ic], (core + 2 * h) * 4 + y)

    above = (x * 4 + z_tm[1] + core, z_sp[1] + y)
    below = (x * 4 + z_tm[7] + core, z_sp[7] + y)
    far_first = (4, 3, 5, 2, 6, 1, 7, 0)
    near_first = (0, 1, 7, 2, 6, 3, 5, 4)
    across = (2, 1, 3, 0)

    def near(cc):
        return div(rem(z - 2 * cc + 9, 8), 4)

    barrier = pltpu.get_barrier_semaphore()

    def greet(dev):
        pl.semaphore_signal(barrier, inc=1, device_id=dev, device_id_type=MESH)

    for iz in far_first:
        for ix in across:
            if ix or iz:
                greet(plane(ix, iz))
    for ih in (1, 0):
        for ix in across:
            for il in (1, 0):
                for ic in (1, 0):
                    if ix or il or ic or ih:
                        greet(origin(ix, il, ic, hs[ih]))
    for iy in across:
        for ix in across:
            for ic in (1, 0):
                if ix or iy or ic:
                    greet(mate(ix, iy, ic))
    greet(above)
    greet(below)

    @pl.when(away)
    def _():
        greet(plane(0, 0))
        greet(origin(0, 0, 0, zhh))

    pl.semaphore_wait(barrier, 97 - 2 * home.astype(jnp.int32))

    def copy_to(src_ref, dst_ref, phase, dev, sem=None):
        return pltpu.make_async_remote_copy(
            src_ref=src_ref, dst_ref=dst_ref, send_sem=send_sem.at[phase],
            recv_sem=recv_sem.at[phase] if sem is None else sem,
            device_id=dev, device_id_type=MESH,
        )

    def wait_on(ref, sem):
        pltpu.make_async_copy(ref, ref, sem).wait()

    def arrived(ref, phase):
        wait_on(ref, recv_sem.at[phase])

    def sent(ref, phase):
        wait_on(ref, send_sem.at[phase])

    for c in loads[:3]:
        c.wait()
    for i in range(2):
        zz = zlo * 4 + core * 2 + i
        here = jnp.logical_and(home, zz == z)
        rows = rsrc.at[zp, pl.ds(2 * zz, 6)]

        @pl.when(here)
        def _():
            pltpu.make_async_copy(rows, r1.at[zhh], recv_sem.at[0]).start()

        @pl.when(jnp.logical_not(here))
        def _():
            dev = (x * 4 + rem(zz, 2) * 2 + par, div(zz, 2) * 4 + y)
            copy_to(rows, r1.at[zhh], 0, dev).start()

    for c in loads[3:]:
        c.wait()

    place = b1.at[zhh, :, pl.ds(2 * tm, 2)]
    b1_sem = recv_sem.at[1 + zhh]

    def piece(ix, iz):
        return src.at[:, :, rem(xs[ix], 2), 2 * zs[iz] + div(xs[ix], 2)]

    @pl.when(home)
    def _():
        pltpu.make_async_copy(piece(0, 0), place, b1_sem).start()

    @pl.when(away)
    def _():
        copy_to(piece(0, 0), place, 1, plane(0, 0), b1_sem).start()

    for iz in near_first:
        for ix in across:
            if ix or iz:
                copy_to(piece(ix, iz), place, 1, plane(ix, iz), b1_sem).start()

    def transform(tile):
        def load(n):
            growth = math.exp(math.log(ALPHA) * n / STEPS)
            return (b1[tile, 0, n] * growth, b1[tile, 1, STEPS - 1 - n] * growth)

        def store(k, v):
            f1[k, tile, 0] = v[0]
            f1[k, tile, 1] = v[1]

        long_dft(load, store, tmp, -1)

    def second(tile, half):
        goal = fld.at[tile, core, y, zp, rtl]
        for iy in across:
            for ix in across:
                for ic in (1, 0):
                    if ix or iy or ic:
                        k = xs[ix] * 8 + ys[iy] * 2 + cs[ic]
                        copy_to(f1.at[k, tile], goal, 4, mate(ix, iy, ic), group_sem.at[half, iy]).start()
        pltpu.make_async_copy(f1.at[freq, tile], goal, group_sem.at[half, 0]).start()

    def shared(half, iy):
        yy = ys[(4 - iy) % 4]
        for cc in range(2):
            tile = near(cc) if half == 0 else 1 - near(cc)
            yield (tile, cc, yy)

    def pass_on(half):
        for iy in (0, 1, 3, 2):
            wait_on(fld.at[0, :, ys[(4 - iy) % 4]], group_sem.at[half, iy])
            for at in shared(half, iy):
                got = fld.at[at]
                copy_to(got.at[:, 0], fha.at[(1,) + at], 5, below).start()
                copy_to(got.at[:, 1], fha.at[(0,) + at], 6, above).start()

    def pass_rest():
        for half in range(2):
            for iy in across:
                for at in shared(half, iy):
                    got = fld.at[at]
                    copy_to(got.at[:, 1, :, pl.ds(0, TAIL)], fhb.at[(1,) + at].at[:, :, :TAIL], 7, below).start()
                    copy_to(got.at[:, 0, :, pl.ds(8 - TAIL, TAIL)], fhb.at[(0,) + at].at[:, :, :TAIL], 8, above).start()

    arrived(r1, 0)
    half_rf = rf.at[:, core]
    beside = rem(x + 1 + 2 * rem(y, 2), 4)
    for iy in across:
        copy_to(r1, half_rf.at[:, y, zp], 3, (beside * 4 + zlo * 2 + core, zhi * 4 + ys[iy])).start()
    for iy in across[:3]:
        copy_to(r1, half_rf.at[:, y, zp], 3, mate(0, iy, 0)).start()
    pltpu.make_async_copy(r1, half_rf.at[:, y, zp], recv_sem.at[3]).start()

    close = near(core)
    arrived(b1.at[0], 1 + close)
    transform(close)
    second(close, 0)

    arrived(rf.at[:, 0], 3)
    copy_to(half_rf, half_rf, 9, mate(0, 0, 1)).start()
    arrived(b1.at[0], 2 - close)
    transform(1 - close)
    second(1 - close, 1)
    pass_on(0)
    arrived(rf.at[:, 0], 9)
    cos_k, sin_k = jnp.float32(0.0), jnp.float32(0.0)
    for k in range(STEPS):
        angle = 2.0 * math.pi * k / STEPS
        cos_k = jnp.where(freq == k, jnp.float32(math.cos(angle)), cos_k)
        sin_k = jnp.where(freq == k, jnp.float32(math.sin(angle)), sin_k)
    rate = math.exp(math.log(ALPHA) / STEPS)
    base_re = 1.0 - rate * cos_k + 6.0
    d_im = rate * sin_k + 1.0

    def coefficient(row, j, value, keep):
        d_re = base_re + value
        inv = 1.0 / (d_re * d_re + d_im * d_im)
        w_re = d_re * inv
        w_im = -d_im * inv
        if keep is not None:
            w_re = jnp.where(keep, w_re, 0.0)
            w_im = jnp.where(keep, w_im, 0.0)
        w[row, 0, j] = w_re
        w[row, 1, j] = w_im

    rfl = rf.reshape(1536, 128)

    def coefficient_row(row, keep):
        for j in range(4):
            value = rfl[pl.ds(j * 48 + row + 16 - HALO, 8, stride=192), :]
            coefficient(row, j, value, keep)

    def coefficient_rows(r, _):
        coefficient_row(HALO + r, None)
        coefficient_row(HALO + 8 + r, None)
        coefficient_row(TAIL + r, z > 0)
        coefficient_row(HALO + 16 + r, z < 7)
        return 0

    lax.fori_loop(0, 8, coefficient_rows, 0)
    for r in range(TAIL):
        coefficient_row(r, z > 0)
        coefficient_row(HALO + 24 + r, z < 7)

    pass_on(1)
    pass_rest()

    fll = fld.reshape(1024, 128)
    fal = fha.reshape(1024, 128)
    fbl = fhb.reshape(1024, 128)

    def start_row(row, j, v):
        s[row, 0, j] = v[0]
        s[row, 1, j] = v[1]
        w_re, w_im = w[row, 0, j], w[row, 1, j]
        u[0, row, 0, j] = w_re * v[0] - w_im * v[1]
        u[0, row, 1, j] = w_re * v[1] + w_im * v[0]

    def inner_start(r, _):
        for t in range(2):
            for j in range(4):
                v = [fll[pl.ds(j * 32 + t * 16 + c * 8 + r, 8, stride=128), :] for c in range(2)]
                start_row(HALO + t * 8 + r, j, v)
        return 0

    lax.fori_loop(0, 8, inner_start, 0)
    lanes = lax.broadcasted_iota(jnp.int32, (8, 128), 1)
    subs = lax.broadcasted_iota(jnp.int32, (8, 128), 0)
    first_lane, last_lane = lanes == 0, lanes == 127
    first_sub, last_sub = subs == 0, subs == 7

    def sweep_row(m, row):
        total = [[None] * 4, [None] * 4]
        for c in range(2):
            mid = [u[m - 1, row, c, j] for j in range(4)]
            before = jnp.where(first_sub, 0.0, pltpu.roll(mid[3], 1, 0))
            after = jnp.where(last_sub, 0.0, pltpu.roll(mid[0], 7, 0))
            line = [before] + mid + [after]
            for j in range(4):
                t = s[row, c, j] + (line[j] + line[j + 2])
                t = t + (u[m - 1, row - 1, c, j] + u[m - 1, row + 1, c, j])
                left = jnp.where(first_lane, 0.0, pltpu.roll(mid[j], 1, 1))
                right = jnp.where(last_lane, 0.0, pltpu.roll(mid[j], 127, 1))
                total[c][j] = t + (left + right)
        for j in range(4):
            w_re, w_im = w[row, 0, j], w[row, 1, j]
            t_re, t_im = total[0][j], total[1][j]
            u[m, row, 0, j] = w_re * t_re - w_im * t_im
            u[m, row, 1, j] = w_re * t_im + w_im * t_re

    done = [set() for _ in range(SWEEPS)]

    def sweeps(edge):
        for m in range(1, SWEEPS):
            rows = set(range(edge + m, ROWS - edge - m)) - done[m]
            done[m] |= rows
            for row in sorted(rows):
                sweep_row(m, row)

    sweeps(HALO)
    for side in range(2):
        arrived(fha.at[side], 6 - side)

    def outer_start(side, row, at, flat):
        for j in range(4):
            first = side * 512 + j * 16 + at
            v = [flat[pl.ds(first + c * 8, 8, stride=64), :] for c in range(2)]
            start_row(row, j, v)

    def wide_start(r, _):
        outer_start(0, TAIL + r, r, fal)
        outer_start(1, HALO + 16 + r, r, fal)
        return 0

    lax.fori_loop(0, 8, wide_start, 0)
    sweeps(TAIL)
    for side in range(2):
        arrived(fhb.at[side, :, :, :, :, :, :TAIL], 8 - side)
    for r in range(TAIL):
        outer_start(0, r, r, fbl)
        outer_start(1, HALO + 24 + r, r, fbl)
    sweeps(0)

    gl = g.reshape(1024, 128)

    def turn_back(r, _):
        for t in range(2):
            for j in range(4):
                for c in range(2):
                    gl[pl.ds(j * 32 + t * 16 + c * 8 + r, 8, stride=128), :] = u[SWEEPS - 1, HALO + t * 8 + r, c, j]
        return 0

    lax.fori_loop(0, 8, turn_back, 0)

    for half in range(2):
        tiles = [1 - near(cc) if half == 0 else near(cc) for cc in cs]
        for iy in across:
            for ix in across:
                for ic in (1, 0):
                    if ix or iy or ic:
                        part = g.at[tiles[ic], cs[ic], ys[iy], rem(xs[ix], 2), div(xs[ix], 2)]
                        copy_to(part, f2.at[tiles[ic], freq], 13, mate(ix, iy, ic), recv_sem.at[14 + half]).start()
        own = g.at[tiles[0], core, y, zp, rtl]
        pltpu.make_async_copy(own, f2.at[tiles[0], freq], recv_sem.at[14 + half]).start()

    def transform_back(tile):
        def load(k):
            return (f2[tile, k, 0], f2[tile, k, 1])

        def store(n, v):
            shrink = math.exp(-math.log(ALPHA) * n / STEPS) / STEPS
            b2[tile, 0, n] = v[0] * shrink
            b2[tile, 1, STEPS - 1 - n] = v[1] * shrink

        long_dft(load, store, tmp, 1)

    goal = out.at[:, :, zp, 2 * z + rtl]

    def fourth(tile):
        for ix in across:
            for il in (1, 0):
                for ic in (1, 0):
                    times = pl.ds(2 * (xs[ix] * 4 + ls[il] * 2 + cs[ic]), 2)
                    part = b2.at[tile, :, times]
                    dev = origin(ix, il, ic, tile)
                    if ix or il or ic:
                        copy_to(part, goal, 16, dev).start()
                    else:
                        here = jnp.logical_and(home, tile == zhh)

                        @pl.when(here)
                        def _():
                            pltpu.make_async_copy(part, goal, recv_sem.at[16]).start()

                        @pl.when(jnp.logical_not(here))
                        def _():
                            copy_to(part, goal, 16, dev).start()

    arrived(f2.at[0], 14)
    transform_back(1 - close)
    fourth(1 - close)
    arrived(f2.at[0], 15)
    transform_back(close)
    fourth(close)

    for i in range(2):
        zz = zlo * 4 + core * 2 + i

        @pl.when(jnp.logical_not(jnp.logical_and(home, zz == z)))
        def _():
            sent(r1.at[0], 0)

    for side in range(2):
        sent(fha.at[side], 6 - side)
        sent(fhb.at[side, :, :, :, :, :, :TAIL], 8 - side)

    sent(rf.at[:, 0], 9)

    def drain_reaction(i, _):
        sent(r1, 3)
        return 0

    lax.fori_loop(1, 8, drain_reaction, 0)

    def drain(i, _):
        sent(b1.at[0, :, pl.ds(0, 2)], 1)
        sent(f1.at[0], 4)
        sent(f1.at[0], 13)
        sent(b1.at[0, :, pl.ds(0, 2)], 16)
        return 0

    lax.fori_loop(1, 32, drain, 0)

    @pl.when(away)
    def _():
        sent(b1.at[0, :, pl.ds(0, 2)], 1)
        sent(b1.at[0, :, pl.ds(0, 2)], 16)

    arrived(out, 16)


def body(state_rhs, adjoint_rhs, reaction):
    tile = (8, 128)
    planes = (2, 2, 4, 2)
    field = pltpu.VMEM((ROWS, 2, 4) + tile, F32)
    result = pl.pallas_call(
        kernel,
        out_shape=jax.ShapeDtypeStruct((2, 2, 2, 16) + tile, F32),
        in_specs=[pl.BlockSpec(memory_space=pl.ANY)] * 3,
        out_specs=pl.BlockSpec(memory_space=pl.ANY),
        scratch_shapes=[
            pltpu.VMEM((2, 2, 2, 16) + tile, F32),
            pltpu.VMEM((2, 20) + tile, F32),
            pltpu.VMEM((2, 6) + tile, F32),
            pltpu.VMEM(planes + (6,) + tile, F32),
            pltpu.VMEM((2, 2, 32) + tile, F32),
            pltpu.VMEM((32, 2) + tile, F32),
            pltpu.VMEM((32, 2, 2) + tile, F32),
            pltpu.VMEM(planes + (2, 2) + tile, F32),
            pltpu.VMEM((2,) + planes + (2,) + tile, F32),
            pltpu.VMEM((2,) + planes + (2,) + tile, F32),
            field,
            field,
            pltpu.VMEM((SWEEPS, ROWS, 2, 4) + tile, F32),
            pltpu.VMEM(planes + (2, 2) + tile, F32),
            pltpu.VMEM((2, 32, 2) + tile, F32),
            pltpu.VMEM((2, 2, 32) + tile, F32),
            pltpu.SemaphoreType.DMA((5,)),
            pltpu.SemaphoreType.DMA((17,)),
            pltpu.SemaphoreType.DMA((17,)),
            pltpu.SemaphoreType.DMA((2, 4)),
        ],
        compiler_params=pltpu.CompilerParams(collective_id=0, has_side_effects=True),
        name="precondition",
    )(
        state_rhs.reshape((2, 2, 16) + tile),
        adjoint_rhs.reshape((2, 2, 16) + tile),
        reaction.reshape((2, 16) + tile),
    )
    return (result[0].reshape(state_rhs.shape), result[1].reshape(state_rhs.shape))


def solution(mesh):
    placed = P("tm", "space", None, None)
    return jax.shard_map(
        body,
        mesh=mesh,
        in_specs=(placed, placed, P("space", None, None)),
        out_specs=(placed, placed),
        check_vma=False,
    )
```

```python
import math

import jax
import jax.numpy as jnp
from jax import lax
from jax.experimental import pallas as pl
from jax.experimental.pallas import tpu as pltpu
from jax.sharding import PartitionSpec as P

STEPS = 32
SWEEPS = 12
ALPHA = 0.1
MESH = pl.DeviceIdType.MESH
TAIL = 3
HALO = 8 + TAIL
ROWS = 16 + 2 * HALO
F32 = jnp.float32


def rem(a, n):
    return lax.rem(a, jnp.int32(n))


def div(a, n):
    return lax.div(a, jnp.int32(n))


def mul_const(v, c):
    re, im = v
    cr, ci = c.real, c.imag
    if abs(ci) < 1e-12:
        if abs(cr - 1.0) < 1e-12:
            return v
        return (re * cr, im * cr)
    if abs(cr) < 1e-12:
        if abs(ci - 1.0) < 1e-12:
            return (-im, re)
        if abs(ci + 1.0) < 1e-12:
            return (im, -re)
        return (im * (-ci), re * ci)
    return (re * cr - im * ci, re * ci + im * cr)


def add(a, b):
    return (a[0] + b[0], a[1] + b[1])


def sub(a, b):
    return (a[0] - b[0], a[1] - b[1])


def small_dft(values, sign):
    n = len(values)
    if n == 1:
        return values
    even = small_dft(values[0::2], sign)
    odd = small_dft(values[1::2], sign)
    out = [None] * n
    for k in range(n // 2):
        angle = sign * 2.0 * math.pi * k / n
        t = mul_const(odd[k], complex(math.cos(angle), math.sin(angle)))
        out[k] = add(even[k], t)
        out[k + n // 2] = sub(even[k], t)
    return out


def long_dft(load, store, tmp, sign):
    for b in range(8):
        group = small_dft([load(8 * a + b) for a in range(4)], sign)
        for k1 in range(4):
            angle = sign * 2.0 * math.pi * b * k1 / 32
            re, im = mul_const(group[k1], complex(math.cos(angle), math.sin(angle)))
            tmp[8 * k1 + b, 0] = re
            tmp[8 * k1 + b, 1] = im
    for k1 in range(4):
        group = small_dft([(tmp[8 * k1 + b, 0], tmp[8 * k1 + b, 1]) for b in range(8)], sign)
        for k2 in range(8):
            store(k1 + 4 * k2, group[k2])


def kernel(
    state, adjoint, reaction, out,
    src, rsrc, r1, rf, b1, tmp, f1, fld, fha, fhb, s, w, u, g, f2, b2,
    load_sem, send_sem, recv_sem, group_sem,
):
    tm = lax.axis_index("tm")
    sp = lax.axis_index("space")
    x, zlo, core = div(tm, 4), rem(div(tm, 2), 2), rem(tm, 2)
    zhi, y = div(sp, 4), rem(sp, 4)
    z = zhi * 2 + zlo
    zhh, par = div(zhi, 2), rem(zhi, 2)
    zp, rtl = rem(x, 2), div(x, 2)
    freq = x * 8 + y * 2 + core
    home = core == par
    away = jnp.logical_not(home)

    loads = [
        pltpu.make_async_copy(reaction, rsrc.at[:, 2:18], load_sem.at[2]),
        pltpu.make_async_copy(reaction.at[:, 14:16], rsrc.at[:, 0:2], load_sem.at[3]),
        pltpu.make_async_copy(reaction.at[:, 0:2], rsrc.at[:, 18:20], load_sem.at[4]),
        pltpu.make_async_copy(state, src.at[0], load_sem.at[0]),
        pltpu.make_async_copy(adjoint, src.at[1], load_sem.at[1]),
    ]
    for c in loads:
        c.start()

    xs = [rem(x + i, 4) for i in range(4)]
    ys = [rem(y + i, 4) for i in range(4)]
    cs = [core, 1 - core]
    zs = [rem(z + i, 8) for i in range(8)]
    hs = [zhh, 1 - zhh]
    ls = [zlo, 1 - zlo]
    z_tm = [rem(v, 2) * 2 for v in zs]
    z_sp = [div(v, 2) * 4 for v in zs]

    def plane(ix, iz):
        return (xs[ix] * 4 + z_tm[iz] + par, z_sp[iz] + y)

    def mate(ix, iy, ic):
        return (xs[ix] * 4 + zlo * 2 + cs[ic], zhi * 4 + ys[iy])

    def origin(ix, il, ic, h):
        return (xs[ix] * 4 + ls[il] * 2 + cs[ic], (core + 2 * h) * 4 + y)

    above = (x * 4 + z_tm[1] + core, z_sp[1] + y)
    below = (x * 4 + z_tm[7] + core, z_sp[7] + y)
    far_first = (4, 3, 5, 2, 6, 1, 7, 0)
    near_first = (0, 1, 7, 2, 6, 3, 5, 4)
    across = (2, 1, 3, 0)

    def near(cc):
        return div(rem(z - 2 * cc + 9, 8), 4)

    barrier = pltpu.get_barrier_semaphore()

    def greet(dev):
        pl.semaphore_signal(barrier, inc=1, device_id=dev, device_id_type=MESH)

    for iz in far_first:
        for ix in across:
            if ix or iz:
                greet(plane(ix, iz))
    for ih in (1, 0):
        for ix in across:
            for il in (1, 0):
                for ic in (1, 0):
                    if ix or il or ic or ih:
                        greet(origin(ix, il, ic, hs[ih]))
    for iy in across:
        for ix in across:
            for ic in (1, 0):
                if ix or iy or ic:
                    greet(mate(ix, iy, ic))
    greet(above)
    greet(below)

    @pl.when(away)
    def _():
        greet(plane(0, 0))
        greet(origin(0, 0, 0, zhh))

    pl.semaphore_wait(barrier, 97 - 2 * home.astype(jnp.int32))

    def copy_to(src_ref, dst_ref, phase, dev, sem=None):
        return pltpu.make_async_remote_copy(
            src_ref=src_ref, dst_ref=dst_ref, send_sem=send_sem.at[phase],
            recv_sem=recv_sem.at[phase] if sem is None else sem,
            device_id=dev, device_id_type=MESH,
        )

    def wait_on(ref, sem):
        pltpu.make_async_copy(ref, ref, sem).wait()

    def arrived(ref, phase):
        wait_on(ref, recv_sem.at[phase])

    def sent(ref, phase):
        wait_on(ref, send_sem.at[phase])

    for c in loads[:3]:
        c.wait()
    for i in range(2):
        zz = zlo * 4 + core * 2 + i
        here = jnp.logical_and(home, zz == z)
        rows = rsrc.at[zp, pl.ds(2 * zz, 6)]

        @pl.when(here)
        def _():
            pltpu.make_async_copy(rows, r1.at[zhh], recv_sem.at[0]).start()

        @pl.when(jnp.logical_not(here))
        def _():
            dev = (x * 4 + rem(zz, 2) * 2 + par, div(zz, 2) * 4 + y)
            copy_to(rows, r1.at[zhh], 0, dev).start()

    for c in loads[3:]:
        c.wait()

    place = b1.at[zhh, :, pl.ds(2 * tm, 2)]
    b1_sem = recv_sem.at[1 + zhh]

    def piece(ix, iz):
        return src.at[:, :, rem(xs[ix], 2), 2 * zs[iz] + div(xs[ix], 2)]

    @pl.when(home)
    def _():
        pltpu.make_async_copy(piece(0, 0), place, b1_sem).start()

    @pl.when(away)
    def _():
        copy_to(piece(0, 0), place, 1, plane(0, 0), b1_sem).start()

    for iz in near_first:
        for ix in across:
            if ix or iz:
                copy_to(piece(ix, iz), place, 1, plane(ix, iz), b1_sem).start()

    def transform(tile):
        def load(n):
            growth = math.exp(math.log(ALPHA) * n / STEPS)
            return (b1[tile, 0, n] * growth, b1[tile, 1, STEPS - 1 - n] * growth)

        def store(k, v):
            f1[k, tile, 0] = v[0]
            f1[k, tile, 1] = v[1]

        long_dft(load, store, tmp, -1)

    def second(tile, half):
        goal = fld.at[tile, core, y, zp, rtl]
        for iy in across:
            for ix in across:
                for ic in (1, 0):
                    if ix or iy or ic:
                        k = xs[ix] * 8 + ys[iy] * 2 + cs[ic]
                        copy_to(f1.at[k, tile], goal, 4, mate(ix, iy, ic), group_sem.at[half, iy]).start()
        pltpu.make_async_copy(f1.at[freq, tile], goal, group_sem.at[half, 0]).start()

    def shared(half, iy):
        yy = ys[(4 - iy) % 4]
        for cc in range(2):
            tile = near(cc) if half == 0 else 1 - near(cc)
            yield (tile, cc, yy)

    def pass_on(half):
        for iy in (0, 1, 3, 2):
            wait_on(fld.at[0, :, ys[(4 - iy) % 4]], group_sem.at[half, iy])
            for at in shared(half, iy):
                got = fld.at[at]
                copy_to(got.at[:, 0], fha.at[(1,) + at], 5, below).start()
                copy_to(got.at[:, 1], fha.at[(0,) + at], 6, above).start()

    def pass_rest():
        for half in range(2):
            for iy in across:
                for at in shared(half, iy):
                    got = fld.at[at]
                    copy_to(got.at[:, 1, :, pl.ds(0, TAIL)], fhb.at[(1,) + at].at[:, :, :TAIL], 7, below).start()
                    copy_to(got.at[:, 0, :, pl.ds(8 - TAIL, TAIL)], fhb.at[(0,) + at].at[:, :, :TAIL], 8, above).start()

    arrived(r1, 0)
    half_rf = rf.at[:, core]
    beside = rem(x + 1 + 2 * rem(y, 2), 4)
    for iy in across:
        copy_to(r1, half_rf.at[:, y, zp], 3, (beside * 4 + zlo * 2 + core, zhi * 4 + ys[iy])).start()
    for iy in across[:3]:
        copy_to(r1, half_rf.at[:, y, zp], 3, mate(0, iy, 0)).start()
    pltpu.make_async_copy(r1, half_rf.at[:, y, zp], recv_sem.at[3]).start()

    close = near(core)
    arrived(b1.at[0], 1 + close)
    transform(close)
    second(close, 0)

    arrived(rf.at[:, 0], 3)
    copy_to(half_rf, half_rf, 9, mate(0, 0, 1)).start()
    arrived(b1.at[0], 2 - close)
    transform(1 - close)
    second(1 - close, 1)
    pass_on(0)
    arrived(rf.at[:, 0], 9)
    cos_k, sin_k = jnp.float32(0.0), jnp.float32(0.0)
    for k in range(STEPS):
        angle = 2.0 * math.pi * k / STEPS
        cos_k = jnp.where(freq == k, jnp.float32(math.cos(angle)), cos_k)
        sin_k = jnp.where(freq == k, jnp.float32(math.sin(angle)), sin_k)
    rate = math.exp(math.log(ALPHA) / STEPS)
    base_re = 1.0 - rate * cos_k + 6.0
    d_im = rate * sin_k + 1.0

    def coefficient(row, j, value, keep):
        d_re = base_re + value
        inv = 1.0 / (d_re * d_re + d_im * d_im)
        w_re = d_re * inv
        w_im = -d_im * inv
        if keep is not None:
            w_re = jnp.where(keep, w_re, 0.0)
            w_im = jnp.where(keep, w_im, 0.0)
        w[row, 0, j] = w_re
        w[row, 1, j] = w_im

    rfl = rf.reshape(1536, 128)

    def coefficient_row(row, keep):
        for j in range(4):
            value = rfl[pl.ds(j * 48 + row + 16 - HALO, 8, stride=192), :]
            coefficient(row, j, value, keep)

    def coefficient_rows(r, _):
        coefficient_row(HALO + r, None)
        coefficient_row(HALO + 8 + r, None)
        coefficient_row(TAIL + r, z > 0)
        coefficient_row(HALO + 16 + r, z < 7)
        return 0

    lax.fori_loop(0, 8, coefficient_rows, 0)
    for r in range(TAIL):
        coefficient_row(r, z > 0)
        coefficient_row(HALO + 24 + r, z < 7)

    pass_on(1)
    pass_rest()

    fll = fld.reshape(1024, 128)
    fal = fha.reshape(1024, 128)
    fbl = fhb.reshape(1024, 128)

    def start_row(row, j, v):
        s[row, 0, j] = v[0]
        s[row, 1, j] = v[1]
        w_re, w_im = w[row, 0, j], w[row, 1, j]
        u[0, row, 0, j] = w_re * v[0] - w_im * v[1]
        u[0, row, 1, j] = w_re * v[1] + w_im * v[0]

    def inner_start(r, _):
        for t in range(2):
            for j in range(4):
                v = [fll[pl.ds(j * 32 + t * 16 + c * 8 + r, 8, stride=128), :] for c in range(2)]
                start_row(HALO + t * 8 + r, j, v)
        return 0

    lax.fori_loop(0, 8, inner_start, 0)
    lanes = lax.broadcasted_iota(jnp.int32, (8, 128), 1)
    subs = lax.broadcasted_iota(jnp.int32, (8, 128), 0)
    first_lane, last_lane = lanes == 0, lanes == 127
    first_sub, last_sub = subs == 0, subs == 7

    gl = g.reshape(1024, 128)

    def sweep_row(m, row):
        total = [[None] * 4, [None] * 4]
        for c in range(2):
            mid = [u[m - 1, row, c, j] for j in range(4)]
            before = jnp.where(first_sub, 0.0, pltpu.roll(mid[3], 1, 0))
            after = jnp.where(last_sub, 0.0, pltpu.roll(mid[0], 7, 0))
            line = [before] + mid + [after]
            for j in range(4):
                t = s[row, c, j] + (line[j] + line[j + 2])
                t = t + (u[m - 1, row - 1, c, j] + u[m - 1, row + 1, c, j])
                left = jnp.where(first_lane, 0.0, pltpu.roll(mid[j], 1, 1))
                right = jnp.where(last_lane, 0.0, pltpu.roll(mid[j], 127, 1))
                total[c][j] = t + (left + right)
        for j in range(4):
            w_re, w_im = w[row, 0, j], w[row, 1, j]
            t_re, t_im = total[0][j], total[1][j]
            new_re, new_im = w_re * t_re - w_im * t_im, w_re * t_im + w_im * t_re
            if m < SWEEPS - 1:
                u[m, row, 0, j] = new_re
                u[m, row, 1, j] = new_im
            else:
                t, r = divmod(row - HALO, 8)
                gl[pl.ds(j * 32 + t * 16 + r, 8, stride=128), :] = new_re
                gl[pl.ds(j * 32 + t * 16 + 8 + r, 8, stride=128), :] = new_im

    done = [set() for _ in range(SWEEPS)]

    def sweeps(edge):
        for m in range(1, SWEEPS):
            rows = set(range(edge + m, ROWS - edge - m)) - done[m]
            done[m] |= rows
            for row in sorted(rows):
                sweep_row(m, row)

    sweeps(HALO)
    for side in range(2):
        arrived(fha.at[side], 6 - side)

    def outer_start(side, row, at, flat):
        for j in range(4):
            first = side * 512 + j * 16 + at
            v = [flat[pl.ds(first + c * 8, 8, stride=64), :] for c in range(2)]
            start_row(row, j, v)

    def wide_start(r, _):
        outer_start(0, TAIL + r, r, fal)
        outer_start(1, HALO + 16 + r, r, fal)
        return 0

    lax.fori_loop(0, 8, wide_start, 0)
    sweeps(TAIL)
    for side in range(2):
        arrived(fhb.at[side, :, :, :, :, :, :TAIL], 8 - side)
    for r in range(TAIL):
        outer_start(0, r, r, fbl)
        outer_start(1, HALO + 24 + r, r, fbl)
    sweeps(0)

    for half in range(2):
        tiles = [1 - near(cc) if half == 0 else near(cc) for cc in cs]
        for iy in across:
            for ix in across:
                for ic in (1, 0):
                    if ix or iy or ic:
                        part = g.at[tiles[ic], cs[ic], ys[iy], rem(xs[ix], 2), div(xs[ix], 2)]
                        copy_to(part, f2.at[tiles[ic], freq], 13, mate(ix, iy, ic), recv_sem.at[14 + half]).start()
        own = g.at[tiles[0], core, y, zp, rtl]
        pltpu.make_async_copy(own, f2.at[tiles[0], freq], recv_sem.at[14 + half]).start()

    def transform_back(tile):
        def load(k):
            return (f2[tile, k, 0], f2[tile, k, 1])

        def store(n, v):
            shrink = math.exp(-math.log(ALPHA) * n / STEPS) / STEPS
            b2[tile, 0, n] = v[0] * shrink
            b2[tile, 1, STEPS - 1 - n] = v[1] * shrink

        long_dft(load, store, tmp, 1)

    goal = out.at[:, :, zp, 2 * z + rtl]

    def fourth(tile):
        for ix in across:
            for il in (1, 0):
                for ic in (1, 0):
                    times = pl.ds(2 * (xs[ix] * 4 + ls[il] * 2 + cs[ic]), 2)
                    part = b2.at[tile, :, times]
                    dev = origin(ix, il, ic, tile)
                    if ix or il or ic:
                        copy_to(part, goal, 16, dev).start()
                    else:
                        here = jnp.logical_and(home, tile == zhh)

                        @pl.when(here)
                        def _():
                            pltpu.make_async_copy(part, goal, recv_sem.at[16]).start()

                        @pl.when(jnp.logical_not(here))
                        def _():
                            copy_to(part, goal, 16, dev).start()

    arrived(f2.at[0], 14)
    transform_back(1 - close)
    fourth(1 - close)
    arrived(f2.at[0], 15)
    transform_back(close)
    fourth(close)

    for i in range(2):
        zz = zlo * 4 + core * 2 + i

        @pl.when(jnp.logical_not(jnp.logical_and(home, zz == z)))
        def _():
            sent(r1.at[0], 0)

    for side in range(2):
        sent(fha.at[side], 6 - side)
        sent(fhb.at[side, :, :, :, :, :, :TAIL], 8 - side)

    sent(rf.at[:, 0], 9)

    def drain_reaction(i, _):
        sent(r1, 3)
        return 0

    lax.fori_loop(1, 8, drain_reaction, 0)

    def drain(i, _):
        sent(b1.at[0, :, pl.ds(0, 2)], 1)
        sent(f1.at[0], 4)
        sent(f1.at[0], 13)
        sent(b1.at[0, :, pl.ds(0, 2)], 16)
        return 0

    lax.fori_loop(1, 32, drain, 0)

    @pl.when(away)
    def _():
        sent(b1.at[0, :, pl.ds(0, 2)], 1)
        sent(b1.at[0, :, pl.ds(0, 2)], 16)

    arrived(out, 16)


def body(state_rhs, adjoint_rhs, reaction):
    tile = (8, 128)
    planes = (2, 2, 4, 2)
    field = pltpu.VMEM((ROWS, 2, 4) + tile, F32)
    result = pl.pallas_call(
        kernel,
        out_shape=jax.ShapeDtypeStruct((2, 2, 2, 16) + tile, F32),
        in_specs=[pl.BlockSpec(memory_space=pl.ANY)] * 3,
        out_specs=pl.BlockSpec(memory_space=pl.ANY),
        scratch_shapes=[
            pltpu.VMEM((2, 2, 2, 16) + tile, F32),
            pltpu.VMEM((2, 20) + tile, F32),
            pltpu.VMEM((2, 6) + tile, F32),
            pltpu.VMEM(planes + (6,) + tile, F32),
            pltpu.VMEM((2, 2, 32) + tile, F32),
            pltpu.VMEM((32, 2) + tile, F32),
            pltpu.VMEM((32, 2, 2) + tile, F32),
            pltpu.VMEM(planes + (2, 2) + tile, F32),
            pltpu.VMEM((2,) + planes + (2,) + tile, F32),
            pltpu.VMEM((2,) + planes + (2,) + tile, F32),
            field,
            field,
            pltpu.VMEM((SWEEPS - 1, ROWS, 2, 4) + tile, F32),
            pltpu.VMEM(planes + (2, 2) + tile, F32),
            pltpu.VMEM((2, 32, 2) + tile, F32),
            pltpu.VMEM((2, 2, 32) + tile, F32),
            pltpu.SemaphoreType.DMA((5,)),
            pltpu.SemaphoreType.DMA((17,)),
            pltpu.SemaphoreType.DMA((17,)),
            pltpu.SemaphoreType.DMA((2, 4)),
        ],
        compiler_params=pltpu.CompilerParams(collective_id=0, has_side_effects=True),
        name="precondition",
    )(
        state_rhs.reshape((2, 2, 16) + tile),
        adjoint_rhs.reshape((2, 2, 16) + tile),
        reaction.reshape((2, 16) + tile),
    )
    return (result[0].reshape(state_rhs.shape), result[1].reshape(state_rhs.shape))


def solution(mesh):
    placed = P("tm", "space", None, None)
    return jax.shard_map(
        body,
        mesh=mesh,
        in_specs=(placed, placed, P("space", None, None)),
        out_specs=(placed, placed),
        check_vma=False,
    )
```
